32 devices in a mesh: gx: 8 (over z, core), gy: 2 (over y), gz: 2 (over x).
Axes of the slice: x: 2, y: 2, z: 4, core: 2. Of those that a mesh axis runs over, the one named last changes fastest.
Arguments:
- volume: float32 [128, 128, 256], P('gx', 'gy', 'gz'), may hold values from -6 to 6
- weights: float32 [64, 8, 128], P(None, None, 'gx'), may hold values from -0.1875 to 0.1875
- offsets: int32 [64, 8], P(None, 'gx'), may hold values from 0 to 57, as said below
- measured: float32 [64, 128, 256], P('gx', 'gy', 'gz'), may hold values from -6 to 6
Outputs:
- gradient: float32 [128, 128, 256], P('gx', 'gy', 'gz')
- residual: float32 [64, 128, 256], P('gx', 'gy', 'gz')
- misfit: float32 [], replicated
The draws below stay inside these ranges and needn't reach their ends.
Inputs may be any that keep to these rules, and one draw needn't show every extreme that they name: offsets[a, b] shifts angle a on brick b; the values 0 and 57 both occur.
All inputs are finite; a program needn't handle non-finite values.
Results may differ from the reference program's by a relative error of at most 0.0003.
Values sent between devices are 32-bit elements; how exact they have to be, the bound alone decides.
No kernel may reach another device: no remote copies, remote signals or barrier semaphores. Data moves between devices by JAX's collectives and lax.ppermute only.
A program may use at most 64 MiB of HBM per device.

```python
import jax
import jax.numpy as jnp
from jax import lax

CX = 16
CY = 64
ANGLES = 64
TAPS = 8
BRICKS_X = 8
NX = 128
NY = 128
NZ = 256
N_GX = 8


def draw_offsets(key, part):
    first, second, third = jax.random.split(jax.random.fold_in(key, 17), 3)
    count = ANGLES * BRICKS_X
    values = jax.random.randint(first, (count,), 0, CY - TAPS + 2)
    high_pos = jax.random.randint(second, (), 0, count)
    low_pos = (high_pos + 1 + jax.random.randint(third, (), 0, count - 1)) % count
    values = values.at[high_pos].set(CY - TAPS + 1)
    values = values.at[low_pos].set(0)
    return values.reshape(ANGLES, BRICKS_X).astype(jnp.int32)


def levels(stream_key, extent, shards, least, largest):
    loudness, own = 1.0, jax.random.fold_in(stream_key, 6)
    for axis_at, parts in shards:
        draws = jnp.exp(jax.random.uniform(jax.random.fold_in(own, axis_at), (parts,), jnp.float32, least / len(shards), largest / len(shards)))
        loudness = loudness * jnp.repeat(draws, extent[axis_at] // parts).reshape([-1 if axis == axis_at else 1 for axis in range(len(extent))])
    return loudness


def normal_values(own_key, dims, scale, reach, shards=(), dtype=jnp.bfloat16):
    drawn = scale * jax.random.normal(own_key, dims, jnp.float32)
    if shards:
        drawn = drawn * levels(own_key, dims, shards, -0.22, 0.18)
    return jnp.clip(drawn, -reach, reach).astype(dtype)


def setup_inputs(seed: int = 0) -> dict:
    key_list = jax.random.split(jax.random.key(seed), 5)
    volume = normal_values(key_list[0], (NX, NY, NZ), 1.0, 6.0, ((0, 8), (1, 2), (2, 2)), jnp.float32)
    weights = normal_values(key_list[1], (ANGLES, TAPS, NX), (NX * TAPS) ** -0.5, 0.1875, ((2, 8),), jnp.float32)
    offsets = draw_offsets(jax.random.fold_in(key_list[4], 71), 0)
    measured = normal_values(key_list[3], (ANGLES, NY, NZ), 1.0, 6.0, ((0, 8), (1, 2), (2, 2)), jnp.float32)
    return {"volume": volume, "weights": weights, "offsets": offsets, "measured": measured}


def project_brick(vol_brick, w_brick, off_brick):
    wblk = w_brick.reshape(ANGLES // 8, 8, TAPS, CX)
    oblk = off_brick.reshape(ANGLES // 8, 8)

    def one_block(args):
        wb, ob = args
        spread = jnp.einsum('adc,cyz->adyz', wb, vol_brick, precision=lax.Precision.HIGHEST)
        padded = jnp.pad(spread, ((0, 0), (0, 0), (0, CY), (0, 0)))

        def per_angle(plane, shift):
            window = lax.dynamic_slice_in_dim(plane, shift.astype(jnp.int32), NY + TAPS - 1, 1)
            total = jnp.zeros((NY, NZ), jnp.float32)
            for tap in range(TAPS):
                total = total + window[tap, tap:tap + NY]
            return total

        return jax.vmap(per_angle)(padded, ob)

    return lax.map(one_block, (wblk, oblk)).reshape(ANGLES, NY, NZ)


def back_brick(resid, w_brick, off_brick):
    padded = jnp.pad(resid, ((0, 0), (CY, 0), (0, 0)))
    wblk = w_brick.reshape(ANGLES // 8, 8, TAPS, CX)
    oblk = off_brick.reshape(ANGLES // 8, 8)
    rblk = padded.reshape(ANGLES // 8, 8, NY + CY, NZ)

    def one_block(grad, args):
        wb, ob, rb = args

        def per_angle(plane, shift):
            start = (CY - shift - (TAPS - 1)).astype(jnp.int32)
            window = lax.dynamic_slice_in_dim(plane, start, NY + TAPS - 1, 0)
            return jnp.stack([window[TAPS - 1 - tap:TAPS - 1 - tap + NY] for tap in range(TAPS)])

        sheared = jax.vmap(per_angle)(rb, ob)
        grad = grad + jnp.einsum('adc,adyz->cyz', wb, sheared, precision=lax.Precision.HIGHEST)
        return grad, None

    grad, unused = lax.scan(one_block, jnp.zeros((CX, NY, NZ), jnp.float32), (wblk, oblk, rblk))
    return grad


def reference(volume, weights, offsets, measured):
    vols = volume.reshape(N_GX, CX, NY, NZ)
    wts = weights.reshape(ANGLES, TAPS, N_GX, CX).transpose(2, 0, 1, 3)
    offs = offsets.T

    def accumulate(total, args):
        vb, wb, ob = args
        return total + project_brick(vb, wb, ob), None

    projection, unused = lax.scan(accumulate, jnp.zeros((ANGLES, NY, NZ), jnp.float32), (vols, wts, offs))
    residual = projection - measured
    misfit = jnp.sum(residual * residual) / (ANGLES * NY * NZ)

    def backward(args):
        wb, ob = args
        return back_brick(residual, wb, ob)

    gradient = lax.map(backward, (wts, offs)).reshape(NX, NY, NZ)
    return gradient, residual, misfit
```

```python
import functools

import jax
import jax.numpy as jnp
from jax import lax
from jax.experimental import pallas as pl
from jax.experimental.pallas import tpu as pltpu
from jax.sharding import PartitionSpec as P

LANES = 128
SUBS = 8


def split(x):
    high = x.astype(jnp.bfloat16)
    low = (x - high.astype(jnp.float32)).astype(jnp.bfloat16)
    return high, low


def lane_ids(rows):
    return lax.broadcasted_iota(jnp.int32, (rows, LANES), 1)


def swap(x):
    return pltpu.roll(x, LANES // 2, 1)


def unpair(first, second):
    left = lane_ids(first.shape[0]) < LANES // 2
    return jnp.where(left, first, swap(second)), jnp.where(left, swap(first), second)


def pack_kernel(half_rows, vol_ref, meas_ref, w_ref, off_ref, out_ref, flat_ref):
    cols, rows, depth = vol_ref.shape
    share = meas_ref.shape[0]
    angles, taps, _ = w_ref.shape
    peers = out_ref.shape[0]
    deep = depth // peers
    at = 0
    for ref, count in ((vol_ref, cols // 2), (meas_ref, share // 2)):
        for j in range(count):
            pair = jnp.concatenate([ref[j], ref[j + count]], axis=0)
            out_ref[:, at : at + deep, :] = pair.T.reshape(peers, deep, LANES)
            at += deep
    for tap in range(taps):
        flat_ref[:, tap * cols : (tap + 1) * cols] = w_ref[:, tap, :]
    start = pl.multiple_of(lax.axis_index("gy") * half_rows, SUBS)
    part = flat_ref[pl.ds(start, half_rows), :]
    out_ref[:, at : at + half_rows, :] = jnp.broadcast_to(part, (peers, half_rows, LANES))
    at += half_rows
    shift = jnp.broadcast_to(off_ref[...].astype(jnp.float32), (angles, LANES))
    shift = jnp.concatenate([shift, jnp.zeros((LANES - angles, LANES), jnp.float32)], axis=0)
    out_ref[:, at : at + SUBS, :] = jnp.broadcast_to(shift.T[:SUBS], (peers, SUBS, LANES))


def main_kernel(dims, in_ref, out_ref, wf_ref, wb_ref, sh_ref, sq_ref):
    bricks, groups, cols, taps, angles, share, deep = dims
    wide = taps * cols
    piece = angles // groups
    w_at = (cols // 2 + share // 2) * deep
    s_at = w_at + piece
    m_at = (cols // 2) * deep
    quarter = share // 2
    for i in range(bricks):
        w = jnp.concatenate([in_ref[i * groups + h, w_at : w_at + piece, :] for h in range(groups)], axis=0)
        high, low = split(w)
        wf_ref[i, :angles, :wide] = high
        wf_ref[i, :angles, wide:] = high
        wf_ref[i, angles:, :wide] = low
        wf_ref[i, angles:, wide:] = jnp.zeros_like(low)
        high, low = split(w.T)
        wb_ref[i, :wide, :angles] = high
        wb_ref[i, :wide, angles:] = high
        wb_ref[i, wide:, :angles] = low
        wb_ref[i, wide:, angles:] = jnp.zeros_like(low)
        row = in_ref[i * groups, s_at : s_at + SUBS, :]
        sh_ref[i] = jnp.concatenate([row] * (LANES // SUBS), axis=0).T[:angles].astype(jnp.int32)
    sq_ref[...] = jnp.zeros_like(sq_ref)
    lane_a = lane_ids(angles)
    lane_c = lane_ids(cols)

    def pair_of_depths(q, carry):
        zs = [2 * q, 2 * q + 1]
        accs = [jnp.zeros((angles, LANES), jnp.float32) for _ in zs]
        for i in range(bricks):
            blocks = []
            for z in zs:
                first, second = (in_ref[i * groups + h, pl.ds(z, cols // 2, stride=deep), :] for h in range(2))
                x = jnp.concatenate(unpair(first, second), axis=0)
                moved = [x]
                for tap in range(1, taps):
                    moved.append(jnp.where(lane_c < LANES - tap, pltpu.roll(x, LANES - tap, 1), 0.0))
                blocks.append(jnp.concatenate(split(jnp.concatenate(moved, axis=0)), axis=0))
            out = jnp.dot(wf_ref[i], jnp.concatenate(blocks, axis=1), preferred_element_type=jnp.float32)
            out = out[:angles] + out[angles:]
            reach = lane_a + sh_ref[i]
            index = reach & (LANES - 1)
            for k in range(2):
                part = out[:, k * LANES : (k + 1) * LANES]
                part = jnp.take_along_axis(part, index, axis=1, mode="promise_in_bounds")
                accs[k] = accs[k] + jnp.where(reach < LANES, part, 0.0)
        resids = []
        for k, z in enumerate(zs):
            rows = []
            for i in range(bricks):
                first, second = (in_ref[i * groups + h, pl.ds(m_at + z, quarter, stride=deep), :] for h in range(2))
                rows.extend(unpair(first, second))
            resid = accs[k] - jnp.concatenate(rows, axis=0)
            square = resid * resid
            for at in range(0, angles, SUBS):
                sq_ref[...] += square[at : at + SUBS]
            resids.append(resid)
            for i in range(bricks):
                low = resid[i * share : i * share + quarter]
                high = resid[i * share + quarter : (i + 1) * share]
                for h, block in enumerate(unpair(low, high)):
                    out_ref[i * groups + h, pl.ds(m_at + z, quarter, stride=deep), :] = block
        for i in range(bricks):
            back = lane_a - sh_ref[i]
            index = back & (LANES - 1)
            blocks = []
            for k in range(2):
                part = jnp.take_along_axis(resids[k], index, axis=1, mode="promise_in_bounds")
                part = jnp.where(back >= 0, part, 0.0)
                blocks.append(jnp.concatenate(split(part), axis=0))
            out = jnp.dot(wb_ref[i], jnp.concatenate(blocks, axis=1), preferred_element_type=jnp.float32)
            out = out[:wide] + out[wide:]
            for k, z in enumerate(zs):
                part = out[:, k * LANES : (k + 1) * LANES]
                total = part[:cols]
                for tap in range(1, taps):
                    total = total + jnp.where(lane_c >= tap, pltpu.roll(part[tap * cols : (tap + 1) * cols], tap, 1), 0.0)
                for h, block in enumerate(unpair(total[: cols // 2], total[cols // 2 :])):
                    out_ref[i * groups + h, pl.ds(z, cols // 2, stride=deep), :] = block
        return carry

    lax.fori_loop(0, deep // 2, pair_of_depths, 0)
    m_end = m_at + quarter * deep
    for p in range(bricks * groups):
        out_ref[p, m_end : m_end + SUBS, :] = sq_ref[...]


def unpack_kernel(in_ref, grad_ref, res_ref, sq_ref):
    peers = in_ref.shape[0]
    cols, rows, depth = grad_ref.shape
    share = res_ref.shape[0]
    deep = depth // peers
    at = 0
    for ref, count in ((grad_ref, cols // 2), (res_ref, share // 2)):
        for j in range(count):
            both = in_ref[:, at : at + deep, :].reshape(depth, LANES).T
            ref[j] = both[:rows]
            ref[j + count] = both[rows:]
            at += deep
    total = in_ref[0, at : at + SUBS, :]
    for p in range(1, peers):
        total = total + in_ref[p, at : at + SUBS, :]
    sq_ref[...] = total


def butterfly(x, axis):
    count = lax.axis_size(axis)
    step = 1
    while step < count:
        x = x + lax.ppermute(x, axis, [(i, i ^ step) for i in range(count)])
        step *= 2
    return x


def passed_along(x, axis, by):
    count = lax.axis_size(axis)
    pairs = [(i, i + by) for i in range(count) if 0 <= i + by < count]
    return lax.ppermute(x, axis, pairs)


def general(volume, weights, offsets, measured):
    cols, rows, depth = volume.shape
    angles = weights.shape[0]
    taps = weights.shape[1]
    blocks = angles // 8
    shifts = offsets[:, 0]
    wblk = weights.reshape(blocks, 8, taps, cols)
    sblk = shifts.reshape(blocks, 8)

    def project(args):
        wb, sb = args
        spread = jnp.einsum("adc,cyz->adyz", wb, volume, precision=lax.Precision.HIGHEST)
        padded = jnp.pad(spread, ((0, 0), (0, 0), (rows, rows), (0, 0)))

        def project_per_angle(plane, shift):
            window = lax.dynamic_slice_in_dim(plane, shift, 2 * rows + taps - 1, 1)
            total = jnp.zeros((2 * rows, depth), jnp.float32)
            for tap in range(taps):
                total = total + window[tap, tap : tap + 2 * rows]
            return total

        return jax.vmap(project_per_angle)(padded, sb)

    window_rows = lax.map(project, (wblk, sblk)).reshape(angles, 2 * rows, depth)
    lower = window_rows[:, :rows]
    upper = window_rows[:, rows:]
    partial_value = upper + passed_along(lower, "gy", -1)
    summed = lax.psum_scatter(partial_value, "gx", scatter_dimension=0, tiled=True)
    resid_share = summed - measured
    before = passed_along(resid_share, "gy", 1)
    resid_all, before_all = (
        lax.all_gather(resid_share, "gx", axis=0, tiled=True),
        lax.all_gather(before, "gx", axis=0, tiled=True),
    )
    extended = jnp.concatenate([before_all, resid_all], axis=1)
    rblk = extended.reshape(blocks, 8, 2 * rows, depth)

    def backward(grad, args):
        wb, sb, rb = args

        def backward_per_angle(plane, shift):
            start = rows - shift - (taps - 1)
            window = lax.dynamic_slice_in_dim(plane, start, rows + taps - 1, 0)
            return jnp.stack(
                [window[taps - 1 - tap : taps - 1 - tap + rows] for tap in range(taps)]
            )

        sheared = jax.vmap(backward_per_angle)(rb, sb)
        grad = grad + jnp.einsum("adc,adyz->cyz", wb, sheared, precision=lax.Precision.HIGHEST)
        return (grad, None)

    gradient, unused = lax.scan(
        backward, jnp.zeros((cols, rows, depth), jnp.float32), (wblk, sblk, rblk)
    )
    entries = angles * rows * depth * lax.axis_size("gy") * lax.axis_size("gz")
    misfit = lax.psum(jnp.sum(resid_share * resid_share), ("gx", "gy", "gz")) / entries
    return (gradient, resid_share, misfit)


def fits(volume, weights, measured):
    cols, rows, depth = volume.shape
    angles, taps, _ = weights.shape
    groups = lax.axis_size("gy")
    deep, rest = divmod(depth, lax.axis_size("gx") * groups)
    return (
        groups == 2
        and 2 * rows == LANES
        and depth == LANES
        and rest == 0
        and deep == SUBS
        and cols == 2 * SUBS
        and taps * cols == LANES
        and angles == LANES // 2
        and measured.shape[0] == SUBS
    )


def body(volume, weights, offsets, measured):
    cols, rows, depth = volume.shape
    angles, taps, _ = weights.shape
    if not fits(volume, weights, measured):
        return general(volume, weights, offsets, measured)
    share = measured.shape[0]
    bricks = lax.axis_size("gx")
    groups = lax.axis_size("gy")
    peers = bricks * groups
    deep = depth // peers
    piece = angles // groups
    moved = (cols // 2 + share // 2) * deep
    sent = moved + piece + SUBS
    f32 = jnp.float32
    payload = pl.pallas_call(
        functools.partial(pack_kernel, piece),
        out_shape=jax.ShapeDtypeStruct((peers, sent, LANES), f32),
        scratch_shapes=[pltpu.VMEM((angles, LANES), f32)],
        name="pack",
    )(volume, measured, weights, offsets)
    arrived = lax.all_to_all(payload, ("gx", "gy"), 0, 0, tiled=True)
    wide = taps * cols
    dims = (bricks, groups, cols, taps, angles, share, deep)
    payload = pl.pallas_call(
        functools.partial(main_kernel, dims),
        out_shape=jax.ShapeDtypeStruct((peers, moved + SUBS, LANES), f32),
        scratch_shapes=[
            pltpu.VMEM((bricks, 2 * angles, 2 * wide), jnp.bfloat16),
            pltpu.VMEM((bricks, 2 * wide, 2 * angles), jnp.bfloat16),
            pltpu.VMEM((bricks, angles, LANES), jnp.int32),
            pltpu.VMEM((SUBS, LANES), f32),
        ],
        name="both_ways",
    )(arrived)
    arrived = lax.all_to_all(payload, ("gx", "gy"), 0, 0, tiled=True)
    gradient, resid, square = pl.pallas_call(
        unpack_kernel,
        out_shape=(
            jax.ShapeDtypeStruct(volume.shape, f32),
            jax.ShapeDtypeStruct(measured.shape, f32),
            jax.ShapeDtypeStruct((SUBS, LANES), f32),
        ),
        name="unpack",
    )(arrived)
    entries = angles * rows * depth * groups * lax.axis_size("gz")
    misfit = jnp.sum(butterfly(square, "gz")) / entries
    return gradient, resid, misfit


def solution(mesh):
    in_specs = (P("gx", "gy", "gz"), P(None, None, "gx"), P(None, "gx"), P("gx", "gy", "gz"))
    out_specs = (P("gx", "gy", "gz"), P("gx", "gy", "gz"), P())
    return jax.shard_map(body, mesh=mesh, in_specs=in_specs, out_specs=out_specs, check_vma=False)
```

```python
import functools

import jax
import jax.numpy as jnp
from jax import lax
from jax.experimental import pallas as pl
from jax.experimental.pallas import tpu as pltpu
from jax.sharding import PartitionSpec as P

LANES = 128
SUBS = 8


def split(x):
    high = x.astype(jnp.bfloat16)
    low = (x - high.astype(jnp.float32)).astype(jnp.bfloat16)
    return high, low


def lane_ids(rows):
    return lax.broadcasted_iota(jnp.int32, (rows, LANES), 1)


def swap(x):
    return pltpu.roll(x, LANES // 2, 1)


def unpair(first, second):
    left = lane_ids(first.shape[0]) < LANES // 2
    return jnp.where(left, first, swap(second)), jnp.where(left, swap(first), second)


def pack_kernel(half_rows, vol_ref, meas_ref, w_ref, off_ref, out_ref, flat_ref):
    cols, rows, depth = vol_ref.shape
    share = meas_ref.shape[0]
    wide, angles = w_ref.shape
    peers = out_ref.shape[0]
    deep = depth // peers
    at = 0
    for ref, count in ((vol_ref, cols // 2), (meas_ref, share // 2)):
        for j in range(count):
            pair = jnp.concatenate([ref[j], ref[j + count]], axis=0)
            out_ref[:, at : at + deep, :] = pair.T.reshape(peers, deep, LANES)
            at += deep
    flat_ref[...] = w_ref[...].T
    start = pl.multiple_of(lax.axis_index("gy") * half_rows, SUBS)
    part = flat_ref[pl.ds(start, half_rows), :]
    out_ref[:, at : at + half_rows, :] = jnp.broadcast_to(part, (peers, half_rows, LANES))
    at += half_rows
    shift = jnp.concatenate([off_ref[...], jnp.zeros((1, LANES - angles), jnp.int32)], axis=1).astype(jnp.float32)
    out_ref[:, at : at + SUBS, :] = jnp.broadcast_to(shift, (peers, SUBS, LANES))


def main_kernel(dims, in_ref, out_ref, wf_ref, wb_ref, sh_ref, sq_ref):
    bricks, groups, cols, taps, angles, share, deep = dims
    wide = taps * cols
    piece = angles // groups
    w_at = (cols // 2 + share // 2) * deep
    s_at = w_at + piece
    m_at = (cols // 2) * deep
    quarter = share // 2
    for i in range(bricks):
        w = jnp.concatenate([in_ref[i * groups + h, w_at : w_at + piece, :] for h in range(groups)], axis=0)
        high, low = split(w)
        wf_ref[i, :angles, :wide] = high
        wf_ref[i, :angles, wide:] = high
        wf_ref[i, angles:, :wide] = low
        wf_ref[i, angles:, wide:] = jnp.zeros_like(low)
        high, low = split(w.T)
        wb_ref[i, :wide, :angles] = high
        wb_ref[i, :wide, angles:] = high
        wb_ref[i, wide:, :angles] = low
        wb_ref[i, wide:, angles:] = jnp.zeros_like(low)
        row = in_ref[i * groups, s_at : s_at + SUBS, :]
        sh_ref[i] = jnp.concatenate([row] * (LANES // SUBS), axis=0).T[:angles].astype(jnp.int32)
    sq_ref[...] = jnp.zeros_like(sq_ref)
    lane_a = lane_ids(angles)
    lane_c = lane_ids(cols)

    def pair_of_depths(q, carry):
        zs = [2 * q, 2 * q + 1]
        accs = [jnp.zeros((angles, LANES), jnp.float32) for _ in zs]
        for i in range(bricks):
            blocks = []
            for z in zs:
                first, second = (in_ref[i * groups + h, pl.ds(z, cols // 2, stride=deep), :] for h in range(2))
                x = jnp.concatenate(unpair(first, second), axis=0)
                moved = [x]
                for tap in range(1, taps):
                    moved.append(jnp.where(lane_c < LANES - tap, pltpu.roll(x, LANES - tap, 1), 0.0))
                blocks.append(jnp.concatenate(split(jnp.concatenate(moved, axis=0)), axis=0))
            out = jnp.dot(wf_ref[i], jnp.concatenate(blocks, axis=1), preferred_element_type=jnp.float32)
            out = out[:angles] + out[angles:]
            reach = lane_a + sh_ref[i]
            index = reach & (LANES - 1)
            for k in range(2):
                part = out[:, k * LANES : (k + 1) * LANES]
                part = jnp.take_along_axis(part, index, axis=1, mode="promise_in_bounds")
                accs[k] = accs[k] + jnp.where(reach < LANES, part, 0.0)
        resids = []
        for k, z in enumerate(zs):
            rows = []
            for i in range(bricks):
                first, second = (in_ref[i * groups + h, pl.ds(m_at + z, quarter, stride=deep), :] for h in range(2))
                rows.extend(unpair(first, second))
            resid = accs[k] - jnp.concatenate(rows, axis=0)
            square = resid * resid
            for at in range(0, angles, SUBS):
                sq_ref[...] += square[at : at + SUBS]
            resids.append(resid)
            for i in range(bricks):
                low = resid[i * share : i * share + quarter]
                high = resid[i * share + quarter : (i + 1) * share]
                for h, block in enumerate(unpair(low, high)):
                    out_ref[i * groups + h, pl.ds(m_at + z, quarter, stride=deep), :] = block
        for i in range(bricks):
            back = lane_a - sh_ref[i]
            index = back & (LANES - 1)
            blocks = []
            for k in range(2):
                part = jnp.take_along_axis(resids[k], index, axis=1, mode="promise_in_bounds")
                part = jnp.where(back >= 0, part, 0.0)
                blocks.append(jnp.concatenate(split(part), axis=0))
            out = jnp.dot(wb_ref[i], jnp.concatenate(blocks, axis=1), preferred_element_type=jnp.float32)
            out = out[:wide] + out[wide:]
            for k, z in enumerate(zs):
                part = out[:, k * LANES : (k + 1) * LANES]
                total = part[:cols]
                for tap in range(1, taps):
                    total = total + jnp.where(lane_c >= tap, pltpu.roll(part[tap * cols : (tap + 1) * cols], tap, 1), 0.0)
                for h, block in enumerate(unpair(total[: cols // 2], total[cols // 2 :])):
                    out_ref[i * groups + h, pl.ds(z, cols // 2, stride=deep), :] = block
        return carry

    lax.fori_loop(0, deep // 2, pair_of_depths, 0)
    m_end = m_at + quarter * deep
    for p in range(bricks * groups):
        out_ref[p, m_end : m_end + SUBS, :] = sq_ref[...]


def unpack_kernel(in_ref, grad_ref, res_ref):
    peers = in_ref.shape[0]
    cols, rows, depth = grad_ref.shape
    share = res_ref.shape[0]
    deep = depth // peers
    at = 0
    for ref, count in ((grad_ref, cols // 2), (res_ref, share // 2)):
        for j in range(count):
            both = in_ref[:, at : at + deep, :].reshape(depth, LANES).T
            ref[j] = both[:rows]
            ref[j + count] = both[rows:]
            at += deep


def butterfly(x, axis):
    count = lax.axis_size(axis)
    step = 1
    while step < count:
        x = x + lax.ppermute(x, axis, [(i, i ^ step) for i in range(count)])
        step *= 2
    return x


def passed_along(x, axis, by):
    count = lax.axis_size(axis)
    pairs = [(i, i + by) for i in range(count) if 0 <= i + by < count]
    return lax.ppermute(x, axis, pairs)


def general(volume, weights, offsets, measured):
    cols, rows, depth = volume.shape
    angles = weights.shape[0]
    taps = weights.shape[1]
    blocks = angles // 8
    shifts = offsets[:, 0]
    wblk = weights.reshape(blocks, 8, taps, cols)
    sblk = shifts.reshape(blocks, 8)

    def project(args):
        wb, sb = args
        spread = jnp.einsum("adc,cyz->adyz", wb, volume, precision=lax.Precision.HIGHEST)
        padded = jnp.pad(spread, ((0, 0), (0, 0), (rows, rows), (0, 0)))

        def project_per_angle(plane, shift):
            window = lax.dynamic_slice_in_dim(plane, shift, 2 * rows + taps - 1, 1)
            total = jnp.zeros((2 * rows, depth), jnp.float32)
            for tap in range(taps):
                total = total + window[tap, tap : tap + 2 * rows]
            return total

        return jax.vmap(project_per_angle)(padded, sb)

    window_rows = lax.map(project, (wblk, sblk)).reshape(angles, 2 * rows, depth)
    lower = window_rows[:, :rows]
    upper = window_rows[:, rows:]
    partial_value = upper + passed_along(lower, "gy", -1)
    summed = lax.psum_scatter(partial_value, "gx", scatter_dimension=0, tiled=True)
    resid_share = summed - measured
    before = passed_along(resid_share, "gy", 1)
    resid_all, before_all = (
        lax.all_gather(resid_share, "gx", axis=0, tiled=True),
        lax.all_gather(before, "gx", axis=0, tiled=True),
    )
    extended = jnp.concatenate([before_all, resid_all], axis=1)
    rblk = extended.reshape(blocks, 8, 2 * rows, depth)

    def backward(grad, args):
        wb, sb, rb = args

        def backward_per_angle(plane, shift):
            start = rows - shift - (taps - 1)
            window = lax.dynamic_slice_in_dim(plane, start, rows + taps - 1, 0)
            return jnp.stack(
                [window[taps - 1 - tap : taps - 1 - tap + rows] for tap in range(taps)]
            )

        sheared = jax.vmap(backward_per_angle)(rb, sb)
        grad = grad + jnp.einsum("adc,adyz->cyz", wb, sheared, precision=lax.Precision.HIGHEST)
        return (grad, None)

    gradient, unused = lax.scan(
        backward, jnp.zeros((cols, rows, depth), jnp.float32), (wblk, sblk, rblk)
    )
    entries = angles * rows * depth * lax.axis_size("gy") * lax.axis_size("gz")
    misfit = lax.psum(jnp.sum(resid_share * resid_share), ("gx", "gy", "gz")) / entries
    return (gradient, resid_share, misfit)


def fits(volume, weights, measured):
    cols, rows, depth = volume.shape
    angles, taps, _ = weights.shape
    groups = lax.axis_size("gy")
    deep, rest = divmod(depth, lax.axis_size("gx") * groups)
    return (
        groups == 2
        and 2 * rows == LANES
        and depth == LANES
        and rest == 0
        and deep == SUBS
        and cols == 2 * SUBS
        and taps * cols == LANES
        and angles == LANES // 2
        and measured.shape[0] == SUBS
    )


def body(volume, weights, offsets, measured):
    cols, rows, depth = volume.shape
    angles, taps, _ = weights.shape
    if not fits(volume, weights, measured):
        return general(volume, weights, offsets, measured)
    share = measured.shape[0]
    bricks = lax.axis_size("gx")
    groups = lax.axis_size("gy")
    peers = bricks * groups
    deep = depth // peers
    piece = angles // groups
    moved = (cols // 2 + share // 2) * deep
    sent = moved + piece + SUBS
    f32 = jnp.float32
    payload = pl.pallas_call(
        functools.partial(pack_kernel, piece),
        out_shape=jax.ShapeDtypeStruct((peers, sent, LANES), f32),
        scratch_shapes=[pltpu.VMEM((angles, LANES), f32)],
        name="pack",
    )(volume, measured, weights.transpose(1, 2, 0).reshape(taps * cols, angles), offsets.reshape(1, angles))
    arrived = lax.all_to_all(payload, ("gx", "gy"), 0, 0, tiled=True)
    wide = taps * cols
    dims = (bricks, groups, cols, taps, angles, share, deep)
    payload = pl.pallas_call(
        functools.partial(main_kernel, dims),
        out_shape=jax.ShapeDtypeStruct((peers, moved + SUBS, LANES), f32),
        scratch_shapes=[
            pltpu.VMEM((bricks, 2 * angles, 2 * wide), jnp.bfloat16),
            pltpu.VMEM((bricks, 2 * wide, 2 * angles), jnp.bfloat16),
            pltpu.VMEM((bricks, angles, LANES), jnp.int32),
            pltpu.VMEM((SUBS, LANES), f32),
        ],
        name="both_ways",
    )(arrived)
    arrived = lax.all_to_all(payload, ("gx", "gy"), 0, 0, tiled=True)
    square = butterfly(jnp.sum(arrived[:, moved:]), "gz")
    gradient, resid = pl.pallas_call(
        unpack_kernel,
        out_shape=(jax.ShapeDtypeStruct(volume.shape, f32), jax.ShapeDtypeStruct(measured.shape, f32)),
        cost_estimate=pl.CostEstimate(flops=1 << 24, bytes_accessed=1 << 21, transcendentals=0),
        name="unpack",
    )(arrived)
    entries = angles * rows * depth * groups * lax.axis_size("gz")
    misfit = square / entries
    return gradient, resid, misfit


def solution(mesh):
    in_specs = (P("gx", "gy", "gz"), P(None, None, "gx"), P(None, "gx"), P("gx", "gy", "gz"))
    out_specs = (P("gx", "gy", "gz"), P("gx", "gy", "gz"), P())
    return jax.shard_map(body, mesh=mesh, in_specs=in_specs, out_specs=out_specs, check_vma=False)
```

```python
import functools

import jax
import jax.numpy as jnp
from jax import lax
from jax.experimental import pallas as pl
from jax.experimental.pallas import tpu as pltpu
from jax.sharding import PartitionSpec as P

LANES = 128
SUBS = 8
STRIDE = 72
TOGETHER = 2


def split(x):
    high = x.astype(jnp.bfloat16)
    low = (x - high.astype(jnp.float32)).astype(jnp.bfloat16)
    return high, low


def lane_ids(rows):
    return lax.broadcasted_iota(jnp.int32, (rows, LANES), 1)


def swap(x):
    return pltpu.roll(x, LANES // 2, 1)


def unpair(first, second):
    left = lane_ids(first.shape[0]) < LANES // 2
    return jnp.where(left, first, swap(second)), jnp.where(left, swap(first), second)


def pack_kernel(half_rows, vol_ref, meas_ref, w_ref, off_ref, out_ref, flat_ref):
    cols, rows, depth = vol_ref.shape
    share = meas_ref.shape[0]
    wide, angles = w_ref.shape
    peers = out_ref.shape[0]
    deep = depth // peers
    at = 0
    for ref, count in ((vol_ref, cols // 2), (meas_ref, share // 2)):
        for j in range(count):
            pair = jnp.concatenate([ref[j], ref[j + count]], axis=0)
            out_ref[:, at : at + deep, :] = pair.T.reshape(peers, deep, LANES)
            at += deep
    flat_ref[...] = w_ref[...].T
    start = pl.multiple_of(lax.axis_index("gy") * half_rows, SUBS)
    part = flat_ref[pl.ds(start, half_rows), :]
    out_ref[:, at : at + half_rows, :] = jnp.broadcast_to(part, (peers, half_rows, LANES))
    at += half_rows
    shift = jnp.concatenate([off_ref[...], jnp.zeros((1, LANES - angles), jnp.int32)], axis=1).astype(jnp.float32)
    out_ref[:, at : at + SUBS, :] = jnp.broadcast_to(shift, (peers, SUBS, LANES))


def three(x):
    high, low = split(x)
    return jnp.concatenate([high, low, high], axis=0)


def main_kernel(dims, in_hbm, out_hbm, *scratch):
    in_ref, out_ref, wf_ref, wb_ref, row_ref, int_ref, sh_ref, total_ref = scratch[:8]
    turn_refs, (in_sem, row_sem, sh_sem, out_sem) = scratch[8 : 8 + TOGETHER], scratch[8 + TOGETHER :]
    bricks, groups, cols, taps, angles, share, deep = dims
    wide = taps * cols
    piece = angles // groups
    half, quarter = cols // 2, share // 2
    m_at = half * deep
    w_at = m_at + quarter * deep
    s_at = w_at + piece

    def from_brick(i):
        return pltpu.make_async_copy(
            in_hbm.at[pl.ds(i * groups, groups)], in_ref.at[pl.ds(i * groups, groups)], in_sem.at[i]
        )

    def shifts_of(i):
        return pltpu.make_async_copy(in_hbm.at[i * groups, pl.ds(s_at, SUBS), :], row_ref.at[i], row_sem.at[i])

    def to_brick(i):
        return pltpu.make_async_copy(
            out_ref.at[pl.ds(i * groups, groups)], out_hbm.at[pl.ds(i * groups, groups)], out_sem.at[i]
        )

    for i in range(bricks):
        shifts_of(i).start()
    for i in range(bricks):
        from_brick(i).start()
    total_ref[...] = jnp.zeros_like(total_ref)
    for i in range(bricks):
        shifts_of(i).wait()
        int_ref[i : i + 1, :] = row_ref[i, :1, :].astype(jnp.int32)
    to_scalars = pltpu.make_async_copy(int_ref, sh_ref, sh_sem)
    to_scalars.start()
    lane_c = lane_ids(cols)
    lane = lane_ids(deep)
    zero = jnp.zeros((cols, LANES), jnp.bfloat16)

    def shift_of(i, a):
        return sh_ref[i, a]

    def weights_of(i):
        w = jnp.concatenate([in_ref[i * groups + h, w_at : w_at + piece, :] for h in range(groups)], axis=0)
        high, low = split(w)
        wf_ref[i, :, :wide] = high
        wf_ref[i, :, wide : 2 * wide] = high
        wf_ref[i, :, 2 * wide :] = low
        high, low = split(w.T)
        wb_ref[i, :, :angles] = high
        wb_ref[i, :, angles : 2 * angles] = high
        wb_ref[i, :, 2 * angles :] = low

    def project(i, turn_ref):
        for q in range(deep // 2):
            blocks = []
            for z in (2 * q, 2 * q + 1):
                first, second = (in_ref[i * groups + h, pl.ds(z, half, stride=deep), :] for h in range(2))
                x = jnp.concatenate(unpair(first, second), axis=0)
                parts = []
                for part in split(x):
                    moved = [part]
                    for tap in range(1, taps):
                        moved.append(jnp.where(lane_c < LANES - tap, pltpu.roll(part, LANES - tap, 1), zero))
                    parts.append(jnp.concatenate(moved, axis=0))
                high, low = parts
                blocks.append(jnp.concatenate([high, low, high], axis=0))
            out = jnp.dot(wf_ref[i], jnp.concatenate(blocks, axis=1), preferred_element_type=jnp.float32)
            for k in range(2):
                at = (2 * q + k) * STRIDE
                turn_ref[at : at + angles, :] = out[:, k * LANES : (k + 1) * LANES]

    def gather_rows(i, turn_refs):
        for a in range(angles):
            part = total_ref[a]
            for k, turn_ref in enumerate(turn_refs):
                shift = shift_of(i + k, a)
                moved = pltpu.roll(turn_ref[pl.ds(a, deep, stride=STRIDE), :], LANES - shift, 1)
                part = part + jnp.where(lane < LANES - shift, moved, 0.0)
            total_ref[a] = part

    def forward(n, carry):
        i = n * TOGETHER
        for k, turn_ref in enumerate(turn_refs):
            from_brick(i + k).wait()
            weights_of(i + k)
            project(i + k, turn_ref)

        @pl.when(n == 0)
        def _():
            to_scalars.wait()

        gather_rows(i, turn_refs)
        return carry

    def scatter_rows(i, turn_ref):
        for a in range(angles):
            shift = shift_of(i, a)
            turn_ref[pl.ds(a, deep, stride=STRIDE), :] = jnp.where(lane >= shift, pltpu.roll(total_ref[a], shift, 1), 0.0)

    def backproject(i, turn_ref):
        for q in range(deep // 2):
            zs = (2 * q, 2 * q + 1)
            blocks = [three(turn_ref[z * STRIDE : z * STRIDE + angles, :]) for z in zs]
            out = jnp.dot(wb_ref[i], jnp.concatenate(blocks, axis=1), preferred_element_type=jnp.float32)
            for k, z in enumerate(zs):
                part = out[:, k * LANES : (k + 1) * LANES]
                total = part[:cols]
                for tap in range(1, taps):
                    total = total + jnp.where(lane_c >= tap, pltpu.roll(part[tap * cols : (tap + 1) * cols], tap, 1), 0.0)
                for h, block in enumerate(unpair(total[:half], total[half:])):
                    out_ref[i * groups + h, pl.ds(z, half, stride=deep), :] = block

    def backward(n, carry):
        i = n * TOGETHER
        for k, turn_ref in enumerate(turn_refs):
            scatter_rows(i + k, turn_ref)
        for k, turn_ref in enumerate(turn_refs):
            backproject(i + k, turn_ref)
        for k in range(TOGETHER):
            to_brick(i + k).start()
        return carry

    lax.fori_loop(0, bricks // TOGETHER, forward, 0)
    square = jnp.zeros((deep, LANES), jnp.float32)
    for i in range(bricks):
        for j in range(quarter):
            at = m_at + j * deep
            low_at, high_at = i * share + j, i * share + quarter + j
            low, high = unpair(*(in_ref[i * groups + h, at : at + deep, :] for h in range(2)))
            low, high = total_ref[low_at] - low, total_ref[high_at] - high
            total_ref[low_at], total_ref[high_at] = low, high
            square = square + low * low + high * high
            for h, block in enumerate(unpair(low, high)):
                out_ref[i * groups + h, at : at + deep, :] = block
    for p in range(bricks * groups):
        out_ref[p, w_at : w_at + deep, :] = square
    lax.fori_loop(0, bricks // TOGETHER, backward, 0)
    for i in range(bricks):
        to_brick(i).wait()


def main_scratch(dims):
    bricks, groups, cols, taps, angles, share, deep = dims
    wide = taps * cols
    f32, bf16 = jnp.float32, jnp.bfloat16
    rows = (cols // 2 + share // 2) * deep
    return [
        pltpu.VMEM((bricks * groups, rows + angles // groups + SUBS, LANES), f32),
        pltpu.VMEM((bricks * groups, rows + SUBS, LANES), f32),
        pltpu.VMEM((bricks, angles, 3 * wide), bf16),
        pltpu.VMEM((bricks, wide, 3 * angles), bf16),
        pltpu.VMEM((bricks, SUBS, LANES), f32),
        pltpu.VMEM((bricks, LANES), jnp.int32),
        pltpu.SMEM((bricks, LANES), jnp.int32),
        pltpu.VMEM((angles, deep, LANES), f32),
        *[pltpu.VMEM((deep * STRIDE, LANES), f32) for _ in range(TOGETHER)],
        pltpu.SemaphoreType.DMA((bricks,)),
        pltpu.SemaphoreType.DMA((bricks,)),
        pltpu.SemaphoreType.DMA,
        pltpu.SemaphoreType.DMA((bricks,)),
    ]


def unpack_kernel(in_ref, grad_ref, res_ref):
    peers = in_ref.shape[0]
    cols, rows, depth = grad_ref.shape
    share = res_ref.shape[0]
    deep = depth // peers
    at = 0
    for ref, count in ((grad_ref, cols // 2), (res_ref, share // 2)):
        for j in range(count):
            both = in_ref[:, at : at + deep, :].reshape(depth, LANES).T
            ref[j] = both[:rows]
            ref[j + count] = both[rows:]
            at += deep


def butterfly(x, axis):
    count = lax.axis_size(axis)
    step = 1
    while step < count:
        x = x + lax.ppermute(x, axis, [(i, i ^ step) for i in range(count)])
        step *= 2
    return x


def passed_along(x, axis, by):
    count = lax.axis_size(axis)
    pairs = [(i, i + by) for i in range(count) if 0 <= i + by < count]
    return lax.ppermute(x, axis, pairs)


def general(volume, weights, offsets, measured):
    cols, rows, depth = volume.shape
    angles = weights.shape[0]
    taps = weights.shape[1]
    blocks = angles // 8
    shifts = offsets[:, 0]
    wblk = weights.reshape(blocks, 8, taps, cols)
    sblk = shifts.reshape(blocks, 8)

    def project(args):
        wb, sb = args
        spread = jnp.einsum("adc,cyz->adyz", wb, volume, precision=lax.Precision.HIGHEST)
        padded = jnp.pad(spread, ((0, 0), (0, 0), (rows, rows), (0, 0)))

        def project_per_angle(plane, shift):
            window = lax.dynamic_slice_in_dim(plane, shift, 2 * rows + taps - 1, 1)
            total = jnp.zeros((2 * rows, depth), jnp.float32)
            for tap in range(taps):
                total = total + window[tap, tap : tap + 2 * rows]
            return total

        return jax.vmap(project_per_angle)(padded, sb)

    window_rows = lax.map(project, (wblk, sblk)).reshape(angles, 2 * rows, depth)
    lower = window_rows[:, :rows]
    upper = window_rows[:, rows:]
    partial_value = upper + passed_along(lower, "gy", -1)
    summed = lax.psum_scatter(partial_value, "gx", scatter_dimension=0, tiled=True)
    resid_share = summed - measured
    before = passed_along(resid_share, "gy", 1)
    resid_all, before_all = (
        lax.all_gather(resid_share, "gx", axis=0, tiled=True),
        lax.all_gather(before, "gx", axis=0, tiled=True),
    )
    extended = jnp.concatenate([before_all, resid_all], axis=1)
    rblk = extended.reshape(blocks, 8, 2 * rows, depth)

    def backward(grad, args):
        wb, sb, rb = args

        def backward_per_angle(plane, shift):
            start = rows - shift - (taps - 1)
            window = lax.dynamic_slice_in_dim(plane, start, rows + taps - 1, 0)
            return jnp.stack(
                [window[taps - 1 - tap : taps - 1 - tap + rows] for tap in range(taps)]
            )

        sheared = jax.vmap(backward_per_angle)(rb, sb)
        grad = grad + jnp.einsum("adc,adyz->cyz", wb, sheared, precision=lax.Precision.HIGHEST)
        return (grad, None)

    gradient, unused = lax.scan(
        backward, jnp.zeros((cols, rows, depth), jnp.float32), (wblk, sblk, rblk)
    )
    entries = angles * rows * depth * lax.axis_size("gy") * lax.axis_size("gz")
    misfit = lax.psum(jnp.sum(resid_share * resid_share), ("gx", "gy", "gz")) / entries
    return (gradient, resid_share, misfit)


def fits(volume, weights, measured):
    cols, rows, depth = volume.shape
    angles, taps, _ = weights.shape
    groups = lax.axis_size("gy")
    deep, rest = divmod(depth, lax.axis_size("gx") * groups)
    return (
        groups == 2
        and 2 * rows == LANES
        and depth == LANES
        and rest == 0
        and deep == SUBS
        and cols == 2 * SUBS
        and taps * cols == LANES
        and angles == LANES // 2
        and measured.shape[0] == SUBS
    )


def body(volume, weights, offsets, measured):
    cols, rows, depth = volume.shape
    angles, taps, _ = weights.shape
    if not fits(volume, weights, measured):
        return general(volume, weights, offsets, measured)
    share = measured.shape[0]
    bricks = lax.axis_size("gx")
    groups = lax.axis_size("gy")
    peers = bricks * groups
    deep = depth // peers
    piece = angles // groups
    moved = (cols // 2 + share // 2) * deep
    sent = moved + piece + SUBS
    f32 = jnp.float32
    payload = pl.pallas_call(
        functools.partial(pack_kernel, piece),
        out_shape=jax.ShapeDtypeStruct((peers, sent, LANES), f32),
        scratch_shapes=[pltpu.VMEM((angles, LANES), f32)],
        name="pack",
    )(volume, measured, weights.transpose(1, 2, 0).reshape(taps * cols, angles), offsets.reshape(1, angles))
    arrived = lax.all_to_all(payload, ("gx", "gy"), 0, 0, tiled=True)
    dims = (bricks, groups, cols, taps, angles, share, deep)
    payload = pl.pallas_call(
        functools.partial(main_kernel, dims),
        out_shape=jax.ShapeDtypeStruct((peers, moved + SUBS, LANES), f32),
        in_specs=[pl.BlockSpec(memory_space=pl.ANY)],
        out_specs=pl.BlockSpec(memory_space=pl.ANY),
        scratch_shapes=main_scratch(dims),
        name="both_ways",
    )(arrived)
    arrived = lax.all_to_all(payload, ("gx", "gy"), 0, 0, tiled=True)
    square = butterfly(jnp.sum(arrived[:, moved:]), "gz")
    gradient, resid = pl.pallas_call(
        unpack_kernel,
        out_shape=(jax.ShapeDtypeStruct(volume.shape, f32), jax.ShapeDtypeStruct(measured.shape, f32)),
        cost_estimate=pl.CostEstimate(flops=1 << 24, bytes_accessed=1 << 21, transcendentals=0),
        name="unpack",
    )(arrived)
    entries = angles * rows * depth * groups * lax.axis_size("gz")
    misfit = square / entries
    return gradient, resid, misfit


def solution(mesh):
    in_specs = (P("gx", "gy", "gz"), P(None, None, "gx"), P(None, "gx"), P("gx", "gy", "gz"))
    out_specs = (P("gx", "gy", "gz"), P("gx", "gy", "gz"), P())
    return jax.shard_map(body, mesh=mesh, in_specs=in_specs, out_specs=out_specs, check_vma=False)
```

```python
import functools

import jax
import jax.numpy as jnp
from jax import lax
from jax.experimental import pallas as pl
from jax.experimental.pallas import tpu as pltpu
from jax.sharding import PartitionSpec as P

LANES = 128
SUBS = 8
STRIDE = 72
TOGETHER = 2


def split(x):
    high = x.astype(jnp.bfloat16)
    low = (x - high.astype(jnp.float32)).astype(jnp.bfloat16)
    return high, low


def lane_ids(rows):
    return lax.broadcasted_iota(jnp.int32, (rows, LANES), 1)


def swap(x):
    return pltpu.roll(x, LANES // 2, 1)


def unpair(first, second):
    left = lane_ids(first.shape[0]) < LANES // 2
    return jnp.where(left, first, swap(second)), jnp.where(left, swap(first), second)


def pack_kernel(half_rows, vol_ref, meas_ref, w_ref, off_ref, out_ref, flat_ref):
    cols, rows, depth = vol_ref.shape
    share = meas_ref.shape[0]
    wide, angles = w_ref.shape
    peers = out_ref.shape[0]
    deep = depth // peers
    at = 0
    for ref, count in ((vol_ref, cols // 2), (meas_ref, share // 2)):
        for j in range(count):
            pair = jnp.concatenate([ref[j], ref[j + count]], axis=0)
            out_ref[:, at : at + deep, :] = pair.T.reshape(peers, deep, LANES)
            at += deep
    flat_ref[...] = w_ref[...].T
    start = pl.multiple_of(lax.axis_index("gy") * half_rows, SUBS)
    part = flat_ref[pl.ds(start, half_rows), :]
    out_ref[:, at : at + half_rows, :] = jnp.broadcast_to(part, (peers, half_rows, LANES))
    at += half_rows
    shift = jnp.concatenate([off_ref[...], jnp.zeros((1, LANES - angles), jnp.int32)], axis=1).astype(jnp.float32)
    out_ref[:, at : at + SUBS, :] = jnp.broadcast_to(shift, (peers, SUBS, LANES))


def three(x):
    high, low = split(x)
    return jnp.concatenate([high, low, high], axis=0)


def main_kernel(dims, in_ref, out_ref, *scratch):
    wf_ref, wb_ref, int_ref, sh_ref, total_ref = scratch[:5]
    turn_refs, sh_sem = scratch[5 : 5 + TOGETHER], scratch[5 + TOGETHER]
    bricks, groups, cols, taps, angles, share, deep = dims
    wide = taps * cols
    piece = angles // groups
    half, quarter = cols // 2, share // 2
    m_at = half * deep
    w_at = m_at + quarter * deep
    s_at = w_at + piece

    for i in range(bricks):
        row = in_ref[i * groups, s_at : s_at + 1, :].astype(jnp.int32)
        int_ref[i : i + 1, :] = row
        int_ref[bricks + i : bricks + i + 1, :] = LANES - row
    to_scalars = pltpu.make_async_copy(int_ref, sh_ref, sh_sem)
    to_scalars.start()
    total_ref[...] = jnp.zeros_like(total_ref)
    lane_c = lane_ids(cols)
    lane = lane_ids(deep)
    zero = jnp.zeros((cols, LANES), jnp.bfloat16)

    def weights_of(i):
        w = jnp.concatenate([in_ref[i * groups + h, w_at : w_at + piece, :] for h in range(groups)], axis=0)
        high, low = split(w)
        wf_ref[i, :, :wide] = high
        wf_ref[i, :, wide : 2 * wide] = high
        wf_ref[i, :, 2 * wide :] = low
        high, low = split(w.T)
        wb_ref[i, :, :angles] = high
        wb_ref[i, :, angles : 2 * angles] = high
        wb_ref[i, :, 2 * angles :] = low

    def project(i, turn_ref):
        for q in range(deep // 2):
            blocks = []
            for z in (2 * q, 2 * q + 1):
                first, second = (in_ref[i * groups + h, pl.ds(z, half, stride=deep), :] for h in range(2))
                x = jnp.concatenate(unpair(first, second), axis=0)
                parts = []
                for part in split(x):
                    moved = [part]
                    for tap in range(1, taps):
                        moved.append(jnp.where(lane_c < LANES - tap, pltpu.roll(part, LANES - tap, 1), zero))
                    parts.append(jnp.concatenate(moved, axis=0))
                high, low = parts
                blocks.append(jnp.concatenate([high, low, high], axis=0))
            out = jnp.dot(wf_ref[i], jnp.concatenate(blocks, axis=1), preferred_element_type=jnp.float32)
            for k in range(2):
                at = (2 * q + k) * STRIDE
                turn_ref[at : at + angles, :] = out[:, k * LANES : (k + 1) * LANES]

    def gather_rows(i, turn_refs):
        for a in range(angles):
            part = total_ref[a]
            for k, turn_ref in enumerate(turn_refs):
                reach = sh_ref[bricks + i + k, a]
                moved = pltpu.roll(turn_ref[pl.ds(a, deep, stride=STRIDE), :], reach, 1)
                part = part + jnp.where(lane < reach, moved, 0.0)
            total_ref[a] = part

    def forward(n, carry):
        i = n * TOGETHER
        for k, turn_ref in enumerate(turn_refs):
            weights_of(i + k)
            project(i + k, turn_ref)

        @pl.when(n == 0)
        def _():
            to_scalars.wait()

        gather_rows(i, turn_refs)
        return carry

    def scatter_rows(i, turn_ref):
        for a in range(angles):
            shift = sh_ref[i, a]
            turn_ref[pl.ds(a, deep, stride=STRIDE), :] = jnp.where(lane >= shift, pltpu.roll(total_ref[a], shift, 1), 0.0)

    def backproject(i, turn_ref):
        for q in range(deep // 2):
            zs = (2 * q, 2 * q + 1)
            blocks = [three(turn_ref[z * STRIDE : z * STRIDE + angles, :]) for z in zs]
            out = jnp.dot(wb_ref[i], jnp.concatenate(blocks, axis=1), preferred_element_type=jnp.float32)
            for k, z in enumerate(zs):
                part = out[:, k * LANES : (k + 1) * LANES]
                total = part[:cols]
                for tap in range(1, taps):
                    total = total + jnp.where(lane_c >= tap, pltpu.roll(part[tap * cols : (tap + 1) * cols], tap, 1), 0.0)
                for h, block in enumerate(unpair(total[:half], total[half:])):
                    out_ref[i * groups + h, pl.ds(z, half, stride=deep), :] = block

    def backward(n, carry):
        i = n * TOGETHER
        for k, turn_ref in enumerate(turn_refs):
            scatter_rows(i + k, turn_ref)
        for k, turn_ref in enumerate(turn_refs):
            backproject(i + k, turn_ref)
        return carry

    lax.fori_loop(0, bricks // TOGETHER, forward, 0)
    square = jnp.zeros((deep, LANES), jnp.float32)
    for i in range(bricks):
        for j in range(quarter):
            at = m_at + j * deep
            low_at, high_at = i * share + j, i * share + quarter + j
            low, high = unpair(*(in_ref[i * groups + h, at : at + deep, :] for h in range(2)))
            low, high = total_ref[low_at] - low, total_ref[high_at] - high
            total_ref[low_at], total_ref[high_at] = low, high
            square = square + low * low + high * high
            for h, block in enumerate(unpair(low, high)):
                out_ref[i * groups + h, at : at + deep, :] = block
    for p in range(bricks * groups):
        out_ref[p, w_at : w_at + deep, :] = square
    lax.fori_loop(0, bricks // TOGETHER, backward, 0)


def main_scratch(dims):
    bricks, groups, cols, taps, angles, share, deep = dims
    wide = taps * cols
    f32, bf16 = jnp.float32, jnp.bfloat16
    return [
        pltpu.VMEM((bricks, angles, 3 * wide), bf16),
        pltpu.VMEM((bricks, wide, 3 * angles), bf16),
        pltpu.VMEM((2 * bricks, LANES), jnp.int32),
        pltpu.SMEM((2 * bricks, LANES), jnp.int32),
        pltpu.VMEM((angles, deep, LANES), f32),
        *[pltpu.VMEM((deep * STRIDE, LANES), f32) for _ in range(TOGETHER)],
        pltpu.SemaphoreType.DMA,
    ]


def unpack_kernel(in_ref, grad_ref, res_ref):
    peers = in_ref.shape[0]
    cols, rows, depth = grad_ref.shape
    share = res_ref.shape[0]
    deep = depth // peers
    at = 0
    for ref, count in ((grad_ref, cols // 2), (res_ref, share // 2)):
        for j in range(count):
            both = in_ref[:, at : at + deep, :].reshape(depth, LANES).T
            ref[j] = both[:rows]
            ref[j + count] = both[rows:]
            at += deep


def on_chip(x):
    return pltpu.with_memory_space_constraint(x, pltpu.VMEM)


def butterfly(x, axis):
    count = lax.axis_size(axis)
    step = 1
    while step < count:
        x = x + lax.ppermute(x, axis, [(i, i ^ step) for i in range(count)])
        step *= 2
    return x


def passed_along(x, axis, by):
    count = lax.axis_size(axis)
    pairs = [(i, i + by) for i in range(count) if 0 <= i + by < count]
    return lax.ppermute(x, axis, pairs)


def general(volume, weights, offsets, measured):
    cols, rows, depth = volume.shape
    angles = weights.shape[0]
    taps = weights.shape[1]
    blocks = angles // 8
    shifts = offsets[:, 0]
    wblk = weights.reshape(blocks, 8, taps, cols)
    sblk = shifts.reshape(blocks, 8)

    def project(args):
        wb, sb = args
        spread = jnp.einsum("adc,cyz->adyz", wb, volume, precision=lax.Precision.HIGHEST)
        padded = jnp.pad(spread, ((0, 0), (0, 0), (rows, rows), (0, 0)))

        def project_per_angle(plane, shift):
            window = lax.dynamic_slice_in_dim(plane, shift, 2 * rows + taps - 1, 1)
            total = jnp.zeros((2 * rows, depth), jnp.float32)
            for tap in range(taps):
                total = total + window[tap, tap : tap + 2 * rows]
            return total

        return jax.vmap(project_per_angle)(padded, sb)

    window_rows = lax.map(project, (wblk, sblk)).reshape(angles, 2 * rows, depth)
    lower = window_rows[:, :rows]
    upper = window_rows[:, rows:]
    partial_value = upper + passed_along(lower, "gy", -1)
    summed = lax.psum_scatter(partial_value, "gx", scatter_dimension=0, tiled=True)
    resid_share = summed - measured
    before = passed_along(resid_share, "gy", 1)
    resid_all, before_all = (
        lax.all_gather(resid_share, "gx", axis=0, tiled=True),
        lax.all_gather(before, "gx", axis=0, tiled=True),
    )
    extended = jnp.concatenate([before_all, resid_all], axis=1)
    rblk = extended.reshape(blocks, 8, 2 * rows, depth)

    def backward(grad, args):
        wb, sb, rb = args

        def backward_per_angle(plane, shift):
            start = rows - shift - (taps - 1)
            window = lax.dynamic_slice_in_dim(plane, start, rows + taps - 1, 0)
            return jnp.stack(
                [window[taps - 1 - tap : taps - 1 - tap + rows] for tap in range(taps)]
            )

        sheared = jax.vmap(backward_per_angle)(rb, sb)
        grad = grad + jnp.einsum("adc,adyz->cyz", wb, sheared, precision=lax.Precision.HIGHEST)
        return (grad, None)

    gradient, unused = lax.scan(
        backward, jnp.zeros((cols, rows, depth), jnp.float32), (wblk, sblk, rblk)
    )
    entries = angles * rows * depth * lax.axis_size("gy") * lax.axis_size("gz")
    misfit = lax.psum(jnp.sum(resid_share * resid_share), ("gx", "gy", "gz")) / entries
    return (gradient, resid_share, misfit)


def fits(volume, weights, measured):
    cols, rows, depth = volume.shape
    angles, taps, _ = weights.shape
    groups = lax.axis_size("gy")
    deep, rest = divmod(depth, lax.axis_size("gx") * groups)
    return (
        groups == 2
        and 2 * rows == LANES
        and depth == LANES
        and rest == 0
        and deep == SUBS
        and cols == 2 * SUBS
        and taps * cols == LANES
        and angles == LANES // 2
        and measured.shape[0] == SUBS
    )


def body(volume, weights, offsets, measured):
    cols, rows, depth = volume.shape
    angles, taps, _ = weights.shape
    if not fits(volume, weights, measured):
        return general(volume, weights, offsets, measured)
    share = measured.shape[0]
    bricks = lax.axis_size("gx")
    groups = lax.axis_size("gy")
    peers = bricks * groups
    deep = depth // peers
    piece = angles // groups
    moved = (cols // 2 + share // 2) * deep
    sent = moved + piece + SUBS
    f32 = jnp.float32
    payload = pl.pallas_call(
        functools.partial(pack_kernel, piece),
        out_shape=pltpu.VMEM((peers, sent, LANES), f32),
        scratch_shapes=[pltpu.VMEM((angles, LANES), f32)],
        name="pack",
    )(volume, measured, weights.transpose(1, 2, 0).reshape(taps * cols, angles), offsets.reshape(1, angles))
    arrived = lax.all_to_all(payload, ("gx", "gy"), 0, 0, tiled=True)
    dims = (bricks, groups, cols, taps, angles, share, deep)
    payload = pl.pallas_call(
        functools.partial(main_kernel, dims),
        out_shape=pltpu.VMEM((peers, moved + SUBS, LANES), f32),
        scratch_shapes=main_scratch(dims),
        name="both_ways",
    )(on_chip(arrived))
    arrived = lax.all_to_all(payload, ("gx", "gy"), 0, 0, tiled=True)
    square = butterfly(jnp.sum(arrived[:, moved:]), "gz")
    gradient, resid = pl.pallas_call(
        unpack_kernel,
        out_shape=(jax.ShapeDtypeStruct(volume.shape, f32), jax.ShapeDtypeStruct(measured.shape, f32)),
        cost_estimate=pl.CostEstimate(flops=1 << 24, bytes_accessed=1 << 21, transcendentals=0),
        name="unpack",
    )(on_chip(arrived))
    entries = angles * rows * depth * groups * lax.axis_size("gz")
    misfit = square / entries
    return gradient, resid, misfit


def solution(mesh):
    in_specs = (P("gx", "gy", "gz"), P(None, None, "gx"), P(None, "gx"), P("gx", "gy", "gz"))
    out_specs = (P("gx", "gy", "gz"), P("gx", "gy", "gz"), P())
    return jax.shard_map(body, mesh=mesh, in_specs=in_specs, out_specs=out_specs, check_vma=False)
```

```python
import functools

import jax
import jax.numpy as jnp
from jax import lax
from jax.experimental import pallas as pl
from jax.experimental.pallas import tpu as pltpu
from jax.sharding import PartitionSpec as P


LANES = 128
SUBS = 8
LIMIT = pltpu.CompilerParams(vmem_limit_bytes=8 << 20)
STRIDE = 72
TOGETHER = 2


def split(x):
    high = x.astype(jnp.bfloat16)
    low = (x - high.astype(jnp.float32)).astype(jnp.bfloat16)
    return high, low


def lane_ids(rows):
    return lax.broadcasted_iota(jnp.int32, (rows, LANES), 1)


def swap(x):
    return pltpu.roll(x, LANES // 2, 1)


def unpair(first, second):
    left = lane_ids(first.shape[0]) < LANES // 2
    return jnp.where(left, first, swap(second)), jnp.where(left, swap(first), second)


def share_kernel(w_ref, off_ref, out_ref):
    angles = w_ref.shape[1]
    out_ref[:angles, :] = w_ref[...].T
    shift = jnp.concatenate([off_ref[...], jnp.zeros((1, LANES - angles), jnp.int32)], axis=1).astype(jnp.float32)
    out_ref[angles:, :] = jnp.broadcast_to(shift, (SUBS, LANES))


def pack_kernel(vol_ref, meas_ref, out_ref):
    cols, _, depth = vol_ref.shape
    share = meas_ref.shape[0]
    peers = out_ref.shape[0]
    deep = depth // peers
    at = 0
    for ref, count in ((vol_ref, cols // 2), (meas_ref, share // 2)):
        for j in range(count):
            pair = jnp.concatenate([ref[j], ref[j + count]], axis=0)
            out_ref[:, at : at + deep, :] = pair.T.reshape(peers, deep, LANES)
            at += deep


def prepare_kernel(in_ref, wf_ref, wb_ref, sh_ref):
    rows, wide = in_ref.shape[-2:]
    bricks = sh_ref.shape[0] // 2
    angles = rows - SUBS
    mine = lax.axis_index("gx")
    plane = lax.axis_index("gy") * 2 + lax.axis_index("gz")
    for c in range(2):
        for y in range(2):
            for x in range(2):
                i = mine ^ c ^ (2 * (plane ^ (2 * y + x)))
                w = in_ref[c, y, x, :angles, :]
                high, low = split(w)
                wf_ref[i, :, :wide] = high
                wf_ref[i, :, wide : 2 * wide] = high
                wf_ref[i, :, 2 * wide :] = low
                high, low = split(w.T)
                wb_ref[i, :, :angles] = high
                wb_ref[i, :, angles : 2 * angles] = high
                wb_ref[i, :, 2 * angles :] = low
                row = in_ref[c, y, x, angles : angles + 1, :].astype(jnp.int32)
                sh_ref[pl.ds(i, 1), :] = row
                sh_ref[pl.ds(bricks + i, 1), :] = LANES - row


def three(x):
    high, low = split(x)
    return jnp.concatenate([high, low, high], axis=0)


def main_kernel(dims, in_ref, wf_ref, wb_ref, int_ref, out_ref, *scratch):
    sh_ref, total_ref = scratch[:2]
    turn_refs, sh_sem = scratch[2 : 2 + TOGETHER], scratch[2 + TOGETHER]
    bricks, groups, cols, taps, angles, share, deep = dims
    half, quarter = cols // 2, share // 2
    m_at = half * deep
    w_at = m_at + quarter * deep

    to_scalars = pltpu.make_async_copy(int_ref, sh_ref, sh_sem)
    to_scalars.start()
    total_ref[...] = jnp.zeros_like(total_ref)
    lane_c = lane_ids(cols)
    lane = lane_ids(deep)
    zero = jnp.zeros((cols, LANES), jnp.bfloat16)

    def project(i, turn_ref):
        for q in range(deep // 2):
            blocks = []
            for z in (2 * q, 2 * q + 1):
                first, second = (in_ref[i * groups + h, pl.ds(z, half, stride=deep), :] for h in range(2))
                x = jnp.concatenate(unpair(first, second), axis=0)
                parts = []
                for part in split(x):
                    moved = [part]
                    for tap in range(1, taps):
                        moved.append(jnp.where(lane_c < LANES - tap, pltpu.roll(part, LANES - tap, 1), zero))
                    parts.append(jnp.concatenate(moved, axis=0))
                high, low = parts
                blocks.append(jnp.concatenate([high, low, high], axis=0))
            out = jnp.dot(wf_ref[i], jnp.concatenate(blocks, axis=1), preferred_element_type=jnp.float32)
            for k in range(2):
                at = (2 * q + k) * STRIDE
                turn_ref[at : at + angles, :] = out[:, k * LANES : (k + 1) * LANES]

    def gather_rows(i, turn_refs):
        for a in range(angles):
            part = total_ref[a]
            for k, turn_ref in enumerate(turn_refs):
                reach = sh_ref[bricks + i + k, a]
                moved = pltpu.roll(turn_ref[pl.ds(a, deep, stride=STRIDE), :], reach, 1)
                part = part + jnp.where(lane < reach, moved, 0.0)
            total_ref[a] = part

    def forward(n, carry):
        i = n * TOGETHER
        for k, turn_ref in enumerate(turn_refs):
            project(i + k, turn_ref)

        @pl.when(n == 0)
        def _():
            to_scalars.wait()

        gather_rows(i, turn_refs)
        return carry

    def scatter_rows(i, turn_ref):
        for a in range(angles):
            shift = sh_ref[i, a]
            turn_ref[pl.ds(a, deep, stride=STRIDE), :] = jnp.where(lane >= shift, pltpu.roll(total_ref[a], shift, 1), 0.0)

    def backproject(i, turn_ref):
        for q in range(deep // 2):
            zs = (2 * q, 2 * q + 1)
            blocks = [three(turn_ref[z * STRIDE : z * STRIDE + angles, :]) for z in zs]
            out = jnp.dot(wb_ref[i], jnp.concatenate(blocks, axis=1), preferred_element_type=jnp.float32)
            for k, z in enumerate(zs):
                part = out[:, k * LANES : (k + 1) * LANES]
                total = part[:cols]
                for tap in range(1, taps):
                    total = total + jnp.where(lane_c >= tap, pltpu.roll(part[tap * cols : (tap + 1) * cols], tap, 1), 0.0)
                for h, block in enumerate(unpair(total[:half], total[half:])):
                    out_ref[i * groups + h, pl.ds(z, half, stride=deep), :] = block

    def backward(n, carry):
        i = n * TOGETHER
        for k, turn_ref in enumerate(turn_refs):
            scatter_rows(i + k, turn_ref)
        for k, turn_ref in enumerate(turn_refs):
            backproject(i + k, turn_ref)
        return carry

    lax.fori_loop(0, bricks // TOGETHER, forward, 0)
    square = jnp.zeros((deep, LANES), jnp.float32)
    for i in range(bricks):
        for j in range(quarter):
            at = m_at + j * deep
            low_at, high_at = i * share + j, i * share + quarter + j
            low, high = unpair(*(in_ref[i * groups + h, at : at + deep, :] for h in range(2)))
            low, high = total_ref[low_at] - low, total_ref[high_at] - high
            total_ref[low_at], total_ref[high_at] = low, high
            square = square + low * low + high * high
            for h, block in enumerate(unpair(low, high)):
                out_ref[i * groups + h, at : at + deep, :] = block
    for p in range(bricks * groups):
        out_ref[p, w_at : w_at + deep, :] = square
    lax.fori_loop(0, bricks // TOGETHER, backward, 0)


def main_scratch(dims):
    bricks, _, _, _, angles, _, deep = dims
    f32 = jnp.float32
    return [
        pltpu.SMEM((2 * bricks, LANES), jnp.int32),
        pltpu.VMEM((angles, deep, LANES), f32),
        *[pltpu.VMEM((deep * STRIDE, LANES), f32) for _ in range(TOGETHER)],
        pltpu.SemaphoreType.DMA,
    ]


def unpack_kernel(in_ref, grad_ref, res_ref):
    peers = in_ref.shape[0]
    cols, rows, depth = grad_ref.shape
    share = res_ref.shape[0]
    deep = depth // peers
    at = 0
    for ref, count in ((grad_ref, cols // 2), (res_ref, share // 2)):
        for j in range(count):
            both = in_ref[:, at : at + deep, :].reshape(depth, LANES).T
            ref[j] = both[:rows]
            ref[j + count] = both[rows:]
            at += deep


def cost(flops):
    return pl.CostEstimate(flops=flops, bytes_accessed=1 << 21, transcendentals=0)


def off_chip(x):
    return pltpu.with_memory_space_constraint(x, pltpu.HBM)


def on_chip(x):
    return pltpu.with_memory_space_constraint(x, pltpu.VMEM)


def over_planes(x):
    sizes = [lax.axis_size(axis) for axis in ("gx", "gy", "gz")]
    planes = sizes[1] * sizes[2]
    pairs = [(at * planes + q, (at ^ (2 * q)) * planes + q) for at in range(sizes[0]) for q in range(planes)]
    return lax.ppermute(x, ("gx", "gy", "gz"), pairs)


def butterfly(x, axis):
    count = lax.axis_size(axis)
    step = 1
    while step < count:
        x = x + lax.ppermute(x, axis, [(i, i ^ step) for i in range(count)])
        step *= 2
    return x


def passed_along(x, axis, by):
    count = lax.axis_size(axis)
    pairs = [(i, i + by) for i in range(count) if 0 <= i + by < count]
    return lax.ppermute(x, axis, pairs)


def general(volume, weights, offsets, measured):
    cols, rows, depth = volume.shape
    angles = weights.shape[0]
    taps = weights.shape[1]
    blocks = angles // 8
    shifts = offsets[:, 0]
    wblk = weights.reshape(blocks, 8, taps, cols)
    sblk = shifts.reshape(blocks, 8)

    def project(args):
        wb, sb = args
        spread = jnp.einsum("adc,cyz->adyz", wb, volume, precision=lax.Precision.HIGHEST)
        padded = jnp.pad(spread, ((0, 0), (0, 0), (rows, rows), (0, 0)))

        def project_per_angle(plane, shift):
            window = lax.dynamic_slice_in_dim(plane, shift, 2 * rows + taps - 1, 1)
            total = jnp.zeros((2 * rows, depth), jnp.float32)
            for tap in range(taps):
                total = total + window[tap, tap : tap + 2 * rows]
            return total

        return jax.vmap(project_per_angle)(padded, sb)

    window_rows = lax.map(project, (wblk, sblk)).reshape(angles, 2 * rows, depth)
    lower = window_rows[:, :rows]
    upper = window_rows[:, rows:]
    partial_value = upper + passed_along(lower, "gy", -1)
    summed = lax.psum_scatter(partial_value, "gx", scatter_dimension=0, tiled=True)
    resid_share = summed - measured
    before = passed_along(resid_share, "gy", 1)
    resid_all, before_all = (
        lax.all_gather(resid_share, "gx", axis=0, tiled=True),
        lax.all_gather(before, "gx", axis=0, tiled=True),
    )
    extended = jnp.concatenate([before_all, resid_all], axis=1)
    rblk = extended.reshape(blocks, 8, 2 * rows, depth)

    def backward(grad, args):
        wb, sb, rb = args

        def backward_per_angle(plane, shift):
            start = rows - shift - (taps - 1)
            window = lax.dynamic_slice_in_dim(plane, start, rows + taps - 1, 0)
            return jnp.stack(
                [window[taps - 1 - tap : taps - 1 - tap + rows] for tap in range(taps)]
            )

        sheared = jax.vmap(backward_per_angle)(rb, sb)
        grad = grad + jnp.einsum("adc,adyz->cyz", wb, sheared, precision=lax.Precision.HIGHEST)
        return (grad, None)

    gradient, _ = lax.scan(
        backward, jnp.zeros((cols, rows, depth), jnp.float32), (wblk, sblk, rblk)
    )
    entries = angles * rows * depth * lax.axis_size("gy") * lax.axis_size("gz")
    misfit = lax.psum(jnp.sum(resid_share * resid_share), ("gx", "gy", "gz")) / entries
    return (gradient, resid_share, misfit)


def fits(volume, weights, measured):
    cols, rows, depth = volume.shape
    angles, taps, _ = weights.shape
    groups = lax.axis_size("gy")
    deep, rest = divmod(depth, lax.axis_size("gx") * groups)
    return (
        groups == 2
        and lax.axis_size("gz") == 2
        and lax.axis_size("gx") == 8
        and 2 * rows == LANES
        and depth == LANES
        and rest == 0
        and deep == SUBS
        and cols == 2 * SUBS
        and taps * cols == LANES
        and angles == LANES // 2
        and measured.shape[0] == SUBS
    )


def body(volume, weights, offsets, measured):
    cols, rows, depth = volume.shape
    angles, taps, _ = weights.shape
    if not fits(volume, weights, measured):
        return general(volume, weights, offsets, measured)
    share = measured.shape[0]
    bricks = lax.axis_size("gx")
    groups = lax.axis_size("gy")
    peers = bricks * groups
    deep = depth // peers
    moved = (cols // 2 + share // 2) * deep
    f32 = jnp.float32
    wide = taps * cols
    part = pl.pallas_call(
        share_kernel,
        out_shape=pltpu.VMEM((angles + SUBS, wide), f32),
        compiler_params=LIMIT, name="share",
    )(off_chip(weights.transpose(1, 2, 0).reshape(wide, angles)), off_chip(offsets.reshape(1, angles)))
    part = over_planes(part)
    payload = pl.pallas_call(
        pack_kernel, out_shape=pltpu.VMEM((peers, moved, LANES), f32), cost_estimate=cost(1 << 24), compiler_params=LIMIT, name="pack"
    )(off_chip(volume), off_chip(measured))
    arrived = lax.all_to_all(payload, ("gx", "gy"), 0, 0, tiled=True)
    for axis in ("gz", "gy", "gx"):
        pairs = [(i, i ^ 1) for i in range(lax.axis_size(axis))]
        part = jnp.stack([part, lax.ppermute(part, axis, pairs)])
    prepared = pl.pallas_call(
        prepare_kernel,
        out_shape=(
            pltpu.VMEM((bricks, angles, 3 * wide), jnp.bfloat16),
            pltpu.VMEM((bricks, wide, 3 * angles), jnp.bfloat16),
            pltpu.VMEM((2 * bricks, LANES), jnp.int32),
        ),
        cost_estimate=cost(1 << 26),
        compiler_params=LIMIT, name="prepare",
    )(on_chip(part))
    dims = (bricks, groups, cols, taps, angles, share, deep)
    payload = pl.pallas_call(
        functools.partial(main_kernel, dims),
        out_shape=pltpu.VMEM((peers, moved + SUBS, LANES), f32),
        scratch_shapes=main_scratch(dims),
        compiler_params=LIMIT, name="both_ways",
    )(on_chip(arrived), *map(on_chip, prepared))
    arrived = lax.all_to_all(payload, ("gx", "gy"), 0, 0, tiled=True)
    square = butterfly(jnp.sum(arrived[:, moved:]), "gz")
    gradient, resid = pl.pallas_call(
        unpack_kernel,
        out_shape=(jax.ShapeDtypeStruct(volume.shape, f32), jax.ShapeDtypeStruct(measured.shape, f32)),
        cost_estimate=cost(1 << 24),
        compiler_params=LIMIT, name="unpack",
    )(on_chip(arrived))
    entries = angles * rows * depth * groups * lax.axis_size("gz")
    misfit = square / entries
    return gradient, resid, misfit


def solution(mesh):
    in_specs = (P("gx", "gy", "gz"), P(None, None, "gx"), P(None, "gx"), P("gx", "gy", "gz"))
    out_specs = (P("gx", "gy", "gz"), P("gx", "gy", "gz"), P())
    return jax.shard_map(body, mesh=mesh, in_specs=in_specs, out_specs=out_specs, check_vma=False)
```

```python
import functools

import jax
import jax.numpy as jnp
from jax import lax
from jax.experimental import pallas as pl
from jax.experimental.pallas import tpu as pltpu
from jax.sharding import PartitionSpec as P


LANES = 128
SUBS = 8
LIMIT = pltpu.CompilerParams(vmem_limit_bytes=8 << 20)
STRIDE = 72
TOGETHER = 2


def split(x):
    high = x.astype(jnp.bfloat16)
    low = (x - high.astype(jnp.float32)).astype(jnp.bfloat16)
    return high, low


def lane_ids(rows):
    return lax.broadcasted_iota(jnp.int32, (rows, LANES), 1)


def swap(x):
    return pltpu.roll(x, LANES // 2, 1)


def parted(first, second):
    left = lane_ids(first.shape[0]) < LANES // 2
    return jnp.where(left, first, second), swap(jnp.where(left, second, first))


def joined(low, high):
    left = lane_ids(low.shape[0]) < LANES // 2
    high = swap(high)
    return jnp.where(left, low, high), jnp.where(left, high, low)


def pack_kernel(vol_ref, meas_ref, w_ref, off_ref, out_ref, part_ref):
    cols, _, depth = vol_ref.shape
    share = meas_ref.shape[0]
    angles = w_ref.shape[1]
    peers = out_ref.shape[0]
    deep = depth // peers
    second = lax.axis_index("gy")
    part_ref[:angles, :] = w_ref[...].T
    shift = jnp.concatenate([off_ref[...], jnp.zeros((1, LANES - angles), jnp.int32)], axis=1).astype(jnp.float32)
    part_ref[angles:, :] = jnp.broadcast_to(shift, (SUBS, LANES))
    at = 0
    for ref, count in ((vol_ref, cols // 2), (meas_ref, share // 2)):
        for j in range(count):
            pair = jnp.concatenate([ref[j + second * count], ref[j + (1 - second) * count]], axis=0)
            out_ref[:, at : at + deep, :] = pair.T.reshape(peers, deep, LANES)
            at += deep


def prepare_kernel(in_ref, wf_ref, wb_ref, sh_ref):
    rows, wide = in_ref.shape[-2:]
    bricks = sh_ref.shape[0] // 2
    angles = rows - SUBS
    mine = lax.axis_index("gx")
    plane = lax.axis_index("gy") * 2 + lax.axis_index("gz")
    for c in range(2):
        for y in range(2):
            for x in range(2):
                i = mine ^ c ^ (2 * (plane ^ (2 * y + x)))
                w = in_ref[c, y, x, :angles, :]
                high, low = split(w)
                wf_ref[i, :angles, :wide] = high
                wf_ref[i, :angles, wide:] = high
                wf_ref[i, angles:, :wide] = low
                wf_ref[i, angles:, wide:] = jnp.zeros_like(low)
                high, low = split(w.T)
                wb_ref[i, :, :angles] = high
                wb_ref[i, :, angles : 2 * angles] = high
                wb_ref[i, :, 2 * angles :] = low
                row = in_ref[c, y, x, angles : angles + 1, :].astype(jnp.int32)
                sh_ref[pl.ds(i, 1), :] = row
                sh_ref[pl.ds(bricks + i, 1), :] = LANES - row


def three(x):
    high, low = split(x)
    return jnp.concatenate([high, low, high], axis=0)


def main_kernel(dims, in_ref, wf_ref, wb_ref, int_ref, out_ref, *scratch):
    sh_ref, total_ref = scratch[:2]
    turn_refs, sh_sem = scratch[2 : 2 + TOGETHER], scratch[2 + TOGETHER]
    bricks, groups, cols, taps, angles, share, deep = dims
    half, quarter = cols // 2, share // 2
    m_at = half * deep
    w_at = m_at + quarter * deep

    to_scalars = pltpu.make_async_copy(int_ref, sh_ref, sh_sem)
    to_scalars.start()
    total_ref[...] = jnp.zeros_like(total_ref)
    lane_c = lane_ids(cols)
    lane = lane_ids(deep)
    zero = jnp.zeros((cols, LANES), jnp.bfloat16)

    def project(i, turn_ref):
        for q in range(deep // 2):
            blocks = []
            for z in (2 * q, 2 * q + 1):
                first, second = (in_ref[i * groups + h, pl.ds(z, half, stride=deep), :] for h in range(2))
                x = jnp.concatenate(parted(first, second), axis=0)
                parts = []
                for part in split(x):
                    moved = [part]
                    for tap in range(1, taps):
                        moved.append(jnp.where(lane_c < LANES - tap, pltpu.roll(part, LANES - tap, 1), zero))
                    parts.append(jnp.concatenate(moved, axis=0))
                blocks.append(jnp.concatenate(parts, axis=0))
            out = jnp.dot(wf_ref[i], jnp.concatenate(blocks, axis=1), preferred_element_type=jnp.float32)
            out = out[:angles] + out[angles:]
            for k in range(2):
                at = (2 * q + k) * STRIDE
                turn_ref[at : at + angles, :] = out[:, k * LANES : (k + 1) * LANES]

    def gather_rows(i, turn_refs):
        for a in range(angles):
            part = total_ref[a]
            for k, turn_ref in enumerate(turn_refs):
                reach = sh_ref[bricks + i + k, a]
                moved = pltpu.roll(turn_ref[pl.ds(a, deep, stride=STRIDE), :], reach, 1)
                part = part + jnp.where(lane < reach, moved, 0.0)
            total_ref[a] = part

    def forward(n, carry):
        i = n * TOGETHER
        for k, turn_ref in enumerate(turn_refs):
            project(i + k, turn_ref)

        @pl.when(n == 0)
        def _():
            to_scalars.wait()

        gather_rows(i, turn_refs)
        return carry

    def scatter_rows(i, turn_ref):
        for a in range(angles):
            shift = sh_ref[i, a]
            turn_ref[pl.ds(a, deep, stride=STRIDE), :] = jnp.where(lane >= shift, pltpu.roll(total_ref[a], shift, 1), 0.0)

    def backproject(i, turn_ref):
        for q in range(deep // 2):
            zs = (2 * q, 2 * q + 1)
            blocks = [three(turn_ref[z * STRIDE : z * STRIDE + angles, :]) for z in zs]
            out = jnp.dot(wb_ref[i], jnp.concatenate(blocks, axis=1), preferred_element_type=jnp.float32)
            for k, z in enumerate(zs):
                part = out[:, k * LANES : (k + 1) * LANES]
                total = part[:cols]
                for tap in range(1, taps):
                    total = total + jnp.where(lane_c >= tap, pltpu.roll(part[tap * cols : (tap + 1) * cols], tap, 1), 0.0)
                for h, block in enumerate(joined(total[:half], total[half:])):
                    out_ref[i * groups + h, pl.ds(z, half, stride=deep), :] = block

    def backward(n, carry):
        i = n * TOGETHER
        for k, turn_ref in enumerate(turn_refs):
            scatter_rows(i + k, turn_ref)
        for k, turn_ref in enumerate(turn_refs):
            backproject(i + k, turn_ref)
        return carry

    lax.fori_loop(0, bricks // TOGETHER, forward, 0)
    square = jnp.zeros((deep, LANES), jnp.float32)
    for i in range(bricks):
        for j in range(quarter):
            at = m_at + j * deep
            low_at, high_at = i * share + j, i * share + quarter + j
            low, high = parted(*(in_ref[i * groups + h, at : at + deep, :] for h in range(2)))
            low, high = total_ref[low_at] - low, total_ref[high_at] - high
            total_ref[low_at], total_ref[high_at] = low, high
            square = square + low * low + high * high
            for h, block in enumerate(joined(low, high)):
                out_ref[i * groups + h, at : at + deep, :] = block
    for p in range(bricks * groups):
        out_ref[p, w_at : w_at + deep, :] = square
    lax.fori_loop(0, bricks // TOGETHER, backward, 0)


def main_scratch(dims):
    bricks, _, _, _, angles, _, deep = dims
    f32 = jnp.float32
    return [
        pltpu.SMEM((2 * bricks, LANES), jnp.int32),
        pltpu.VMEM((angles, deep, LANES), f32),
        *[pltpu.VMEM((deep * STRIDE, LANES), f32) for _ in range(TOGETHER)],
        pltpu.SemaphoreType.DMA,
    ]


def unpack_kernel(in_ref, grad_ref, res_ref):
    peers = in_ref.shape[0]
    cols, rows, depth = grad_ref.shape
    share = res_ref.shape[0]
    deep = depth // peers
    second = lax.axis_index("gy")
    at = 0
    for ref, count in ((grad_ref, cols // 2), (res_ref, share // 2)):
        for j in range(count):
            both = in_ref[:, at : at + deep, :].reshape(depth, LANES).T
            ref[j + second * count] = both[:rows]
            ref[j + (1 - second) * count] = both[rows:]
            at += deep


def cost(flops):
    return pl.CostEstimate(flops=flops, bytes_accessed=1 << 21, transcendentals=0)


def off_chip(x):
    return pltpu.with_memory_space_constraint(x, pltpu.HBM)


def on_chip(x):
    return pltpu.with_memory_space_constraint(x, pltpu.VMEM)


def over_planes(x):
    sizes = [lax.axis_size(axis) for axis in ("gx", "gy", "gz")]
    planes = sizes[1] * sizes[2]
    pairs = [(at * planes + q, (at ^ (2 * q)) * planes + q) for at in range(sizes[0]) for q in range(planes)]
    return lax.ppermute(x, ("gx", "gy", "gz"), pairs)


def butterfly(x, axis):
    count = lax.axis_size(axis)
    step = 1
    while step < count:
        x = x + lax.ppermute(x, axis, [(i, i ^ step) for i in range(count)])
        step *= 2
    return x


def passed_along(x, axis, by):
    count = lax.axis_size(axis)
    pairs = [(i, i + by) for i in range(count) if 0 <= i + by < count]
    return lax.ppermute(x, axis, pairs)


def general(volume, weights, offsets, measured):
    cols, rows, depth = volume.shape
    angles = weights.shape[0]
    taps = weights.shape[1]
    blocks = angles // 8
    shifts = offsets[:, 0]
    wblk = weights.reshape(blocks, 8, taps, cols)
    sblk = shifts.reshape(blocks, 8)

    def project(args):
        wb, sb = args
        spread = jnp.einsum("adc,cyz->adyz", wb, volume, precision=lax.Precision.HIGHEST)
        padded = jnp.pad(spread, ((0, 0), (0, 0), (rows, rows), (0, 0)))

        def project_per_angle(plane, shift):
            window = lax.dynamic_slice_in_dim(plane, shift, 2 * rows + taps - 1, 1)
            total = jnp.zeros((2 * rows, depth), jnp.float32)
            for tap in range(taps):
                total = total + window[tap, tap : tap + 2 * rows]
            return total

        return jax.vmap(project_per_angle)(padded, sb)

    window_rows = lax.map(project, (wblk, sblk)).reshape(angles, 2 * rows, depth)
    lower = window_rows[:, :rows]
    upper = window_rows[:, rows:]
    partial_value = upper + passed_along(lower, "gy", -1)
    summed = lax.psum_scatter(partial_value, "gx", scatter_dimension=0, tiled=True)
    resid_share = summed - measured
    before = passed_along(resid_share, "gy", 1)
    resid_all, before_all = (
        lax.all_gather(resid_share, "gx", axis=0, tiled=True),
        lax.all_gather(before, "gx", axis=0, tiled=True),
    )
    extended = jnp.concatenate([before_all, resid_all], axis=1)
    rblk = extended.reshape(blocks, 8, 2 * rows, depth)

    def backward(grad, args):
        wb, sb, rb = args

        def backward_per_angle(plane, shift):
            start = rows - shift - (taps - 1)
            window = lax.dynamic_slice_in_dim(plane, start, rows + taps - 1, 0)
            return jnp.stack(
                [window[taps - 1 - tap : taps - 1 - tap + rows] for tap in range(taps)]
            )

        sheared = jax.vmap(backward_per_angle)(rb, sb)
        grad = grad + jnp.einsum("adc,adyz->cyz", wb, sheared, precision=lax.Precision.HIGHEST)
        return (grad, None)

    gradient, _ = lax.scan(
        backward, jnp.zeros((cols, rows, depth), jnp.float32), (wblk, sblk, rblk)
    )
    entries = angles * rows * depth * lax.axis_size("gy") * lax.axis_size("gz")
    misfit = lax.psum(jnp.sum(resid_share * resid_share), ("gx", "gy", "gz")) / entries
    return (gradient, resid_share, misfit)


def fits(volume, weights, measured):
    cols, rows, depth = volume.shape
    angles, taps, _ = weights.shape
    groups = lax.axis_size("gy")
    deep, rest = divmod(depth, lax.axis_size("gx") * groups)
    return (
        groups == 2
        and lax.axis_size("gz") == 2
        and lax.axis_size("gx") == 8
        and 2 * rows == LANES
        and depth == LANES
        and rest == 0
        and deep == SUBS
        and cols == 2 * SUBS
        and taps * cols == LANES
        and angles == LANES // 2
        and measured.shape[0] == SUBS
    )


def body(volume, weights, offsets, measured):
    cols, rows, depth = volume.shape
    angles, taps, _ = weights.shape
    if not fits(volume, weights, measured):
        return general(volume, weights, offsets, measured)
    share = measured.shape[0]
    bricks = lax.axis_size("gx")
    groups = lax.axis_size("gy")
    peers = bricks * groups
    deep = depth // peers
    moved = (cols // 2 + share // 2) * deep
    f32 = jnp.float32
    wide = taps * cols
    payload, part = pl.pallas_call(
        pack_kernel,
        out_shape=(pltpu.VMEM((peers, moved, LANES), f32), pltpu.VMEM((angles + SUBS, wide), f32)),
        compiler_params=LIMIT,
        name="pack",
    )(
        off_chip(volume),
        off_chip(measured),
        off_chip(weights.transpose(1, 2, 0).reshape(wide, angles)),
        off_chip(offsets.reshape(1, angles)),
    )
    part = over_planes(part)
    arrived = lax.all_to_all(payload, ("gx", "gy"), 0, 0, tiled=True)
    for axis in ("gz", "gy", "gx"):
        pairs = [(i, i ^ 1) for i in range(lax.axis_size(axis))]
        part = jnp.stack([part, lax.ppermute(part, axis, pairs)])
    prepared = pl.pallas_call(
        prepare_kernel,
        out_shape=(
            pltpu.VMEM((bricks, 2 * angles, 2 * wide), jnp.bfloat16),
            pltpu.VMEM((bricks, wide, 3 * angles), jnp.bfloat16),
            pltpu.VMEM((2 * bricks, LANES), jnp.int32),
        ),
        cost_estimate=cost(1 << 26),
        compiler_params=LIMIT, name="prepare",
    )(on_chip(part))
    dims = (bricks, groups, cols, taps, angles, share, deep)
    payload = pl.pallas_call(
        functools.partial(main_kernel, dims),
        out_shape=pltpu.VMEM((peers, moved + SUBS, LANES), f32),
        scratch_shapes=main_scratch(dims),
        compiler_params=LIMIT, name="both_ways",
    )(on_chip(arrived), *map(on_chip, prepared))
    arrived = lax.all_to_all(payload, ("gx", "gy"), 0, 0, tiled=True)
    square = butterfly(jnp.sum(arrived[:, moved:]), "gz")
    gradient, resid = pl.pallas_call(
        unpack_kernel,
        out_shape=(jax.ShapeDtypeStruct(volume.shape, f32), jax.ShapeDtypeStruct(measured.shape, f32)),
        cost_estimate=cost(1 << 24),
        compiler_params=LIMIT, name="unpack",
    )(on_chip(arrived))
    entries = angles * rows * depth * groups * lax.axis_size("gz")
    misfit = square / entries
    return gradient, resid, misfit


def solution(mesh):
    in_specs = (P("gx", "gy", "gz"), P(None, None, "gx"), P(None, "gx"), P("gx", "gy", "gz"))
    out_specs = (P("gx", "gy", "gz"), P("gx", "gy", "gz"), P())
    return jax.shard_map(body, mesh=mesh, in_specs=in_specs, out_specs=out_specs, check_vma=False)
```

```python
import functools

import jax
import jax.numpy as jnp
from jax import lax
from jax.experimental import pallas as pl
from jax.experimental.pallas import tpu as pltpu
from jax.sharding import PartitionSpec as P


LANES = 128
SUBS = 8
LIMIT = pltpu.CompilerParams(vmem_limit_bytes=8 << 20)
STRIDE = 72
TOGETHER = 4


def split(x):
    high = x.astype(jnp.bfloat16)
    low = (x - high.astype(jnp.float32)).astype(jnp.bfloat16)
    return high, low


def lane_ids(rows):
    return lax.broadcasted_iota(jnp.int32, (rows, LANES), 1)


def swap(x):
    return pltpu.roll(x, LANES // 2, 1)


def parted(first, second):
    left = lane_ids(first.shape[0]) < LANES // 2
    return jnp.where(left, first, second), swap(jnp.where(left, second, first))


def joined(low, high):
    left = lane_ids(low.shape[0]) < LANES // 2
    high = swap(high)
    return jnp.where(left, low, high), jnp.where(left, high, low)


def pack_kernel(vol_ref, meas_ref, w_ref, off_ref, out_ref, part_ref):
    cols, _, depth = vol_ref.shape
    share = meas_ref.shape[0]
    angles = w_ref.shape[1]
    peers = out_ref.shape[0]
    deep = depth // peers
    second = lax.axis_index("gy")
    part_ref[:angles, :] = w_ref[...].T
    shift = jnp.concatenate([off_ref[...], jnp.zeros((1, LANES - angles), jnp.int32)], axis=1).astype(jnp.float32)
    part_ref[angles:, :] = jnp.broadcast_to(shift, (SUBS, LANES))
    at = 0
    for ref, count in ((vol_ref, cols // 2), (meas_ref, share // 2)):
        for j in range(count):
            pair = jnp.concatenate([ref[j + second * count], ref[j + (1 - second) * count]], axis=0)
            out_ref[:, at : at + deep, :] = pair.T.reshape(peers, deep, LANES)
            at += deep


def prepare_kernel(in_ref, wf_ref, wb_ref, sh_ref):
    rows, wide = in_ref.shape[-2:]
    bricks = sh_ref.shape[0] // 2
    angles = rows - SUBS
    mine = lax.axis_index("gx")
    plane = lax.axis_index("gy") * 2 + lax.axis_index("gz")
    for c in range(2):
        for y in range(2):
            for x in range(2):
                i = mine ^ c ^ (2 * (plane ^ (2 * y + x)))
                w = in_ref[c, y, x, :angles, :]
                high, low = split(w)
                wf_ref[i, :angles, :wide] = high
                wf_ref[i, :angles, wide:] = high
                wf_ref[i, angles:, :wide] = low
                wf_ref[i, angles:, wide:] = jnp.zeros_like(low)
                high, low = split(w.T)
                wb_ref[i, :, :angles] = high
                wb_ref[i, :, angles : 2 * angles] = high
                wb_ref[i, :, 2 * angles :] = low
                row = in_ref[c, y, x, angles : angles + 1, :].astype(jnp.int32)
                sh_ref[pl.ds(i, 1), :] = row
                sh_ref[pl.ds(bricks + i, 1), :] = LANES - row


def three(x):
    high, low = split(x)
    return jnp.concatenate([high, low, high], axis=0)


def main_kernel(dims, in_ref, wf_ref, wb_ref, int_ref, out_ref, *scratch):
    sh_ref, total_ref = scratch[:2]
    turn_refs, sh_sem = scratch[2 : 2 + TOGETHER], scratch[2 + TOGETHER]
    bricks, groups, cols, taps, angles, share, deep = dims
    half, quarter = cols // 2, share // 2
    m_at = half * deep
    w_at = m_at + quarter * deep

    to_scalars = pltpu.make_async_copy(int_ref, sh_ref, sh_sem)
    to_scalars.start()
    total_ref[...] = jnp.zeros_like(total_ref)
    lane_c = lane_ids(cols)
    lane = lane_ids(deep)
    zero = jnp.zeros((cols, LANES), jnp.bfloat16)

    def project(i, turn_ref):
        for q in range(deep // 2):
            blocks = []
            for z in (2 * q, 2 * q + 1):
                first, second = (in_ref[i * groups + h, pl.ds(z, half, stride=deep), :] for h in range(2))
                x = jnp.concatenate(parted(first, second), axis=0)
                parts = []
                for part in split(x):
                    moved = [part]
                    for tap in range(1, taps):
                        moved.append(jnp.where(lane_c < LANES - tap, pltpu.roll(part, LANES - tap, 1), zero))
                    parts.append(jnp.concatenate(moved, axis=0))
                blocks.append(jnp.concatenate(parts, axis=0))
            out = jnp.dot(wf_ref[i], jnp.concatenate(blocks, axis=1), preferred_element_type=jnp.float32)
            out = out[:angles] + out[angles:]
            for k in range(2):
                at = (2 * q + k) * STRIDE
                turn_ref[at : at + angles, :] = out[:, k * LANES : (k + 1) * LANES]

    def gather_rows(i, turn_refs):
        for a in range(angles):
            part = total_ref[a]
            for k, turn_ref in enumerate(turn_refs):
                reach = sh_ref[bricks + i + k, a]
                moved = pltpu.roll(turn_ref[pl.ds(a, deep, stride=STRIDE), :], reach, 1)
                part = part + jnp.where(lane < reach, moved, 0.0)
            total_ref[a] = part

    def forward(n, carry):
        i = n * TOGETHER
        for k, turn_ref in enumerate(turn_refs):
            project(i + k, turn_ref)

        @pl.when(n == 0)
        def _():
            to_scalars.wait()

        gather_rows(i, turn_refs)
        return carry

    def scatter_rows(i, turn_ref):
        for a in range(angles):
            shift = sh_ref[i, a]
            turn_ref[pl.ds(a, deep, stride=STRIDE), :] = jnp.where(lane >= shift, pltpu.roll(total_ref[a], shift, 1), 0.0)

    def backproject(i, turn_ref):
        for q in range(deep // 2):
            zs = (2 * q, 2 * q + 1)
            blocks = [three(turn_ref[z * STRIDE : z * STRIDE + angles, :]) for z in zs]
            out = jnp.dot(wb_ref[i], jnp.concatenate(blocks, axis=1), preferred_element_type=jnp.float32)
            for k, z in enumerate(zs):
                part = out[:, k * LANES : (k + 1) * LANES]
                total = part[:cols]
                for tap in range(1, taps):
                    total = total + jnp.where(lane_c >= tap, pltpu.roll(part[tap * cols : (tap + 1) * cols], tap, 1), 0.0)
                for h, block in enumerate(joined(total[:half], total[half:])):
                    out_ref[i * groups + h, pl.ds(z, half, stride=deep), :] = block

    def backward(n, carry):
        i = 2 * n
        for k in range(2):
            scatter_rows(i + k, turn_refs[k])
            backproject(i + k, turn_refs[k])
        return carry

    lax.fori_loop(0, bricks // TOGETHER, forward, 0)
    square = jnp.zeros((deep, LANES), jnp.float32)
    for i in range(bricks):
        for j in range(quarter):
            at = m_at + j * deep
            low_at, high_at = i * share + j, i * share + quarter + j
            low, high = parted(*(in_ref[i * groups + h, at : at + deep, :] for h in range(2)))
            low, high = total_ref[low_at] - low, total_ref[high_at] - high
            total_ref[low_at], total_ref[high_at] = low, high
            square = square + low * low + high * high
            for h, block in enumerate(joined(low, high)):
                out_ref[i * groups + h, at : at + deep, :] = block
    for p in range(bricks * groups):
        out_ref[p, w_at : w_at + deep, :] = square
    lax.fori_loop(0, bricks // 2, backward, 0)


def main_scratch(dims):
    bricks, _, _, _, angles, _, deep = dims
    f32 = jnp.float32
    return [
        pltpu.SMEM((2 * bricks, LANES), jnp.int32),
        pltpu.VMEM((angles, deep, LANES), f32),
        *[pltpu.VMEM((deep * STRIDE, LANES), f32) for _ in range(TOGETHER)],
        pltpu.SemaphoreType.DMA,
    ]


def unpack_kernel(in_ref, grad_ref, res_ref):
    peers = in_ref.shape[0]
    cols, rows, depth = grad_ref.shape
    share = res_ref.shape[0]
    deep = depth // peers
    second = lax.axis_index("gy")
    at = 0
    for ref, count in ((grad_ref, cols // 2), (res_ref, share // 2)):
        for j in range(count):
            both = in_ref[:, at : at + deep, :].reshape(depth, LANES).T
            ref[j + second * count] = both[:rows]
            ref[j + (1 - second) * count] = both[rows:]
            at += deep


def cost(flops):
    return pl.CostEstimate(flops=flops, bytes_accessed=1 << 21, transcendentals=0)


def off_chip(x):
    return pltpu.with_memory_space_constraint(x, pltpu.HBM)


def on_chip(x):
    return pltpu.with_memory_space_constraint(x, pltpu.VMEM)


def over_planes(x):
    sizes = [lax.axis_size(axis) for axis in ("gx", "gy", "gz")]
    planes = sizes[1] * sizes[2]
    pairs = [(at * planes + q, (at ^ (2 * q)) * planes + q) for at in range(sizes[0]) for q in range(planes)]
    return lax.ppermute(x, ("gx", "gy", "gz"), pairs)


def butterfly(x, axis):
    count = lax.axis_size(axis)
    step = 1
    while step < count:
        x = x + lax.ppermute(x, axis, [(i, i ^ step) for i in range(count)])
        step *= 2
    return x


def passed_along(x, axis, by):
    count = lax.axis_size(axis)
    pairs = [(i, i + by) for i in range(count) if 0 <= i + by < count]
    return lax.ppermute(x, axis, pairs)


def general(volume, weights, offsets, measured):
    cols, rows, depth = volume.shape
    angles = weights.shape[0]
    taps = weights.shape[1]
    blocks = angles // 8
    shifts = offsets[:, 0]
    wblk = weights.reshape(blocks, 8, taps, cols)
    sblk = shifts.reshape(blocks, 8)

    def project(args):
        wb, sb = args
        spread = jnp.einsum("adc,cyz->adyz", wb, volume, precision=lax.Precision.HIGHEST)
        padded = jnp.pad(spread, ((0, 0), (0, 0), (rows, rows), (0, 0)))

        def project_per_angle(plane, shift):
            window = lax.dynamic_slice_in_dim(plane, shift, 2 * rows + taps - 1, 1)
            total = jnp.zeros((2 * rows, depth), jnp.float32)
            for tap in range(taps):
                total = total + window[tap, tap : tap + 2 * rows]
            return total

        return jax.vmap(project_per_angle)(padded, sb)

    window_rows = lax.map(project, (wblk, sblk)).reshape(angles, 2 * rows, depth)
    lower = window_rows[:, :rows]
    upper = window_rows[:, rows:]
    partial_value = upper + passed_along(lower, "gy", -1)
    summed = lax.psum_scatter(partial_value, "gx", scatter_dimension=0, tiled=True)
    resid_share = summed - measured
    before = passed_along(resid_share, "gy", 1)
    resid_all, before_all = (
        lax.all_gather(resid_share, "gx", axis=0, tiled=True),
        lax.all_gather(before, "gx", axis=0, tiled=True),
    )
    extended = jnp.concatenate([before_all, resid_all], axis=1)
    rblk = extended.reshape(blocks, 8, 2 * rows, depth)

    def backward(grad, args):
        wb, sb, rb = args

        def backward_per_angle(plane, shift):
            start = rows - shift - (taps - 1)
            window = lax.dynamic_slice_in_dim(plane, start, rows + taps - 1, 0)
            return jnp.stack(
                [window[taps - 1 - tap : taps - 1 - tap + rows] for tap in range(taps)]
            )

        sheared = jax.vmap(backward_per_angle)(rb, sb)
        grad = grad + jnp.einsum("adc,adyz->cyz", wb, sheared, precision=lax.Precision.HIGHEST)
        return (grad, None)

    gradient, _ = lax.scan(
        backward, jnp.zeros((cols, rows, depth), jnp.float32), (wblk, sblk, rblk)
    )
    entries = angles * rows * depth * lax.axis_size("gy") * lax.axis_size("gz")
    misfit = lax.psum(jnp.sum(resid_share * resid_share), ("gx", "gy", "gz")) / entries
    return (gradient, resid_share, misfit)


def fits(volume, weights, measured):
    cols, rows, depth = volume.shape
    angles, taps, _ = weights.shape
    groups = lax.axis_size("gy")
    deep, rest = divmod(depth, lax.axis_size("gx") * groups)
    return (
        groups == 2
        and lax.axis_size("gz") == 2
        and lax.axis_size("gx") == 8
        and 2 * rows == LANES
        and depth == LANES
        and rest == 0
        and deep == SUBS
        and cols == 2 * SUBS
        and taps * cols == LANES
        and angles == LANES // 2
        and measured.shape[0] == SUBS
    )


def body(volume, weights, offsets, measured):
    cols, rows, depth = volume.shape
    angles, taps, _ = weights.shape
    if not fits(volume, weights, measured):
        return general(volume, weights, offsets, measured)
    share = measured.shape[0]
    bricks = lax.axis_size("gx")
    groups = lax.axis_size("gy")
    peers = bricks * groups
    deep = depth // peers
    moved = (cols // 2 + share // 2) * deep
    f32 = jnp.float32
    wide = taps * cols
    payload, part = pl.pallas_call(
        pack_kernel,
        out_shape=(pltpu.VMEM((peers, moved, LANES), f32), pltpu.VMEM((angles + SUBS, wide), f32)),
        compiler_params=LIMIT,
        name="pack",
    )(
        off_chip(volume),
        off_chip(measured),
        off_chip(weights.transpose(1, 2, 0).reshape(wide, angles)),
        off_chip(offsets.reshape(1, angles)),
    )
    part = over_planes(part)
    arrived = lax.all_to_all(payload, ("gx", "gy"), 0, 0, tiled=True)
    for axis in ("gz", "gy", "gx"):
        pairs = [(i, i ^ 1) for i in range(lax.axis_size(axis))]
        part = jnp.stack([part, lax.ppermute(part, axis, pairs)])
    prepared = pl.pallas_call(
        prepare_kernel,
        out_shape=(
            pltpu.VMEM((bricks, 2 * angles, 2 * wide), jnp.bfloat16),
            pltpu.VMEM((bricks, wide, 3 * angles), jnp.bfloat16),
            pltpu.VMEM((2 * bricks, LANES), jnp.int32),
        ),
        cost_estimate=cost(1 << 26),
        compiler_params=LIMIT, name="prepare",
    )(on_chip(part))
    dims = (bricks, groups, cols, taps, angles, share, deep)
    payload = pl.pallas_call(
        functools.partial(main_kernel, dims),
        out_shape=pltpu.VMEM((peers, moved + SUBS, LANES), f32),
        scratch_shapes=main_scratch(dims),
        compiler_params=LIMIT, name="both_ways",
    )(on_chip(arrived), *map(on_chip, prepared))
    arrived = lax.all_to_all(payload, ("gx", "gy"), 0, 0, tiled=True)
    entries = angles * rows * depth * groups * lax.axis_size("gz")
    misfit = butterfly(jnp.sum(arrived[:, moved:]) / entries, "gz")
    gradient, resid = pl.pallas_call(
        unpack_kernel,
        out_shape=(jax.ShapeDtypeStruct(volume.shape, f32), jax.ShapeDtypeStruct(measured.shape, f32)),
        cost_estimate=cost(1 << 24),
        compiler_params=LIMIT, name="unpack",
    )(on_chip(arrived))
    return gradient, resid, misfit


def solution(mesh):
    in_specs = (P("gx", "gy", "gz"), P(None, None, "gx"), P(None, "gx"), P("gx", "gy", "gz"))
    out_specs = (P("gx", "gy", "gz"), P("gx", "gy", "gz"), P())
    return jax.shard_map(body, mesh=mesh, in_specs=in_specs, out_specs=out_specs, check_vma=False)
```

```python
import functools

import jax
import jax.numpy as jnp
from jax import lax
from jax.experimental import pallas as pl
from jax.experimental.pallas import tpu as pltpu
from jax.sharding import PartitionSpec as P


LANES = 128
SUBS = 8
LIMIT = pltpu.CompilerParams(vmem_limit_bytes=8 << 20)
STRIDE = 72
TOGETHER = 4


def split(x):
    high = x.astype(jnp.bfloat16)
    low = (x - high.astype(jnp.float32)).astype(jnp.bfloat16)
    return high, low


def lane_ids(rows):
    return lax.broadcasted_iota(jnp.int32, (rows, LANES), 1)


def swap(x):
    return pltpu.roll(x, LANES // 2, 1)


def parted(first, second):
    left = lane_ids(first.shape[0]) < LANES // 2
    return jnp.where(left, first, second), swap(jnp.where(left, second, first))


def joined(low, high):
    left = lane_ids(low.shape[0]) < LANES // 2
    high = swap(high)
    return jnp.where(left, low, high), jnp.where(left, high, low)


def pack_kernel(vol_ref, meas_ref, w_ref, off_ref, out_ref, part_ref):
    cols, _, depth = vol_ref.shape
    share = meas_ref.shape[0]
    angles = w_ref.shape[1]
    peers = out_ref.shape[0]
    deep = depth // peers
    second = lax.axis_index("gy")
    part_ref[:angles, :] = w_ref[...].T
    shift = jnp.concatenate([off_ref[...], jnp.zeros((1, LANES - angles), jnp.int32)], axis=1).astype(jnp.float32)
    part_ref[angles:, :] = jnp.broadcast_to(shift, (SUBS, LANES))
    at = 0
    for ref, count in ((vol_ref, cols // 2), (meas_ref, share // 2)):
        for j in range(count):
            pair = jnp.concatenate([ref[j + second * count], ref[j + (1 - second) * count]], axis=0)
            out_ref[:, at : at + deep, :] = pair.T.reshape(peers, deep, LANES)
            at += deep


def prepare_kernel(in_ref, wf_ref, wb_ref, sh_ref):
    rows, wide = in_ref.shape[-2:]
    bricks = sh_ref.shape[0] // 2
    angles = rows - SUBS
    mine = lax.axis_index("gx")
    plane = lax.axis_index("gy") * 2 + lax.axis_index("gz")
    for c in range(2):
        for y in range(2):
            for x in range(2):
                i = mine ^ c ^ (2 * (plane ^ (2 * y + x)))
                w = in_ref[c, y, x, :angles, :]
                high, low = split(w)
                wf_ref[i, :angles, :wide] = high
                wf_ref[i, :angles, wide:] = high
                wf_ref[i, angles:, :wide] = low
                wf_ref[i, angles:, wide:] = jnp.zeros_like(low)
                high, low = split(w.T)
                wb_ref[i, :, :angles] = high
                wb_ref[i, :, angles : 2 * angles] = high
                wb_ref[i, :, 2 * angles :] = low
                row = in_ref[c, y, x, angles : angles + 1, :].astype(jnp.int32)
                sh_ref[pl.ds(i, 1), :] = row
                sh_ref[pl.ds(bricks + i, 1), :] = LANES - row


def three(x):
    high, low = split(x)
    return jnp.concatenate([high, low, high], axis=0)


def main_kernel(dims, in_ref, wf_ref, wb_ref, int_ref, out_ref, *scratch):
    sh_ref, total_ref = scratch[:2]
    turn_refs, sh_sem = scratch[2 : 2 + TOGETHER], scratch[2 + TOGETHER]
    bricks, groups, cols, taps, angles, share, deep = dims
    half, quarter = cols // 2, share // 2
    m_at = half * deep
    w_at = m_at + quarter * deep

    to_scalars = pltpu.make_async_copy(int_ref, sh_ref, sh_sem)
    to_scalars.start()
    total_ref[...] = jnp.zeros_like(total_ref)
    lane_c = lane_ids(cols)
    lane = lane_ids(deep)
    zero = jnp.zeros((cols, LANES), jnp.bfloat16)

    def project(i, turn_ref):
        for q in range(deep // 2):
            blocks = []
            for z in (2 * q, 2 * q + 1):
                first, second = (in_ref[i * groups + h, pl.ds(z, half, stride=deep), :] for h in range(2))
                x = jnp.concatenate(parted(first, second), axis=0)
                parts = []
                for part in split(x):
                    moved = [part]
                    for tap in range(1, taps):
                        moved.append(jnp.where(lane_c < LANES - tap, pltpu.roll(part, LANES - tap, 1), zero))
                    parts.append(jnp.concatenate(moved, axis=0))
                blocks.append(jnp.concatenate(parts, axis=0))
            out = jnp.dot(wf_ref[i], jnp.concatenate(blocks, axis=1), preferred_element_type=jnp.float32)
            out = out[:angles] + out[angles:]
            for k in range(2):
                at = (2 * q + k) * STRIDE
                turn_ref[at : at + angles, :] = out[:, k * LANES : (k + 1) * LANES]

    def gather_rows(i, turn_refs):
        for a in range(angles):
            part = total_ref[a]
            for k, turn_ref in enumerate(turn_refs):
                reach = sh_ref[bricks + i + k, a]
                moved = pltpu.roll(turn_ref[pl.ds(a, deep, stride=STRIDE), :], reach, 1)
                part = part + jnp.where(lane < reach, moved, 0.0)
            total_ref[a] = part

    def forward(n, carry):
        i = n * TOGETHER
        for k, turn_ref in enumerate(turn_refs):
            project(i + k, turn_ref)

        @pl.when(n == 0)
        def _():
            to_scalars.wait()

        gather_rows(i, turn_refs)
        return carry

    def scatter_rows(i, turn_ref):
        for a in range(angles):
            shift = sh_ref[i, a]
            turn_ref[pl.ds(a, deep, stride=STRIDE), :] = jnp.where(lane >= shift, pltpu.roll(total_ref[a], shift, 1), 0.0)

    def backproject(i, turn_ref):
        for q in range(deep // 2):
            zs = (2 * q, 2 * q + 1)
            blocks = [three(turn_ref[z * STRIDE : z * STRIDE + angles, :]) for z in zs]
            out = jnp.dot(wb_ref[i], jnp.concatenate(blocks, axis=1), preferred_element_type=jnp.float32)
            for k, z in enumerate(zs):
                part = out[:, k * LANES : (k + 1) * LANES]
                total = part[:cols]
                for tap in range(1, taps):
                    total = total + jnp.where(lane_c >= tap, pltpu.roll(part[tap * cols : (tap + 1) * cols], tap, 1), 0.0)
                for h, block in enumerate(joined(total[:half], total[half:])):
                    out_ref[i * groups + h, pl.ds(z, half, stride=deep), :] = block

    def backward(n, carry):
        i = 2 * n
        for k in range(2):
            scatter_rows(i + k, turn_refs[k])
            backproject(i + k, turn_refs[k])
        return carry

    lax.fori_loop(0, bricks // TOGETHER, forward, 0)
    square = jnp.zeros((deep, LANES), jnp.float32)
    for i in range(bricks):
        for j in range(quarter):
            at = m_at + j * deep
            low_at, high_at = i * share + j, i * share + quarter + j
            low, high = parted(*(in_ref[i * groups + h, at : at + deep, :] for h in range(2)))
            low, high = total_ref[low_at] - low, total_ref[high_at] - high
            total_ref[low_at], total_ref[high_at] = low, high
            square = square + low * low + high * high
            for h, block in enumerate(joined(low, high)):
                out_ref[i * groups + h, at : at + deep, :] = block
    for p in range(bricks * groups):
        out_ref[p, w_at : w_at + deep, :] = square
    lax.fori_loop(0, bricks // 2, backward, 0)


def main_scratch(dims):
    bricks, _, _, _, angles, _, deep = dims
    f32 = jnp.float32
    return [
        pltpu.SMEM((2 * bricks, LANES), jnp.int32),
        pltpu.VMEM((angles, deep, LANES), f32),
        *[pltpu.VMEM((deep * STRIDE, LANES), f32) for _ in range(TOGETHER)],
        pltpu.SemaphoreType.DMA,
    ]


def unpack(in_ref, at, out_ref):
    peers = in_ref.shape[0]
    count, rows, depth = out_ref.shape
    deep = depth // peers
    second = lax.axis_index("gy")
    for j in range(count // 2):
        both = in_ref[:, at : at + deep, :].reshape(depth, LANES).T
        out_ref[j + second * (count // 2)] = both[:rows]
        out_ref[j + (1 - second) * (count // 2)] = both[rows:]
        at += deep


def gradient_kernel(in_ref, grad_ref):
    unpack(in_ref, 0, grad_ref)


def residual_kernel(entries, in_ref, own_ref, other_ref, res_ref, misfit_ref):
    cut = in_ref.shape[1] - SUBS
    unpack(in_ref, cut - res_ref.shape[0] // 2 * (res_ref.shape[2] // in_ref.shape[0]), res_ref)
    misfit_ref[...] = jnp.sum(own_ref[...] + other_ref[...], keepdims=True) / entries


def cost(flops):
    return pl.CostEstimate(flops=flops, bytes_accessed=1 << 21, transcendentals=0)


def off_chip(x):
    return pltpu.with_memory_space_constraint(x, pltpu.HBM)


def on_chip(x):
    return pltpu.with_memory_space_constraint(x, pltpu.VMEM)


def over_planes(x):
    sizes = [lax.axis_size(axis) for axis in ("gx", "gy", "gz")]
    planes = sizes[1] * sizes[2]
    pairs = [(at * planes + q, (at ^ (2 * q)) * planes + q) for at in range(sizes[0]) for q in range(planes)]
    return lax.ppermute(x, ("gx", "gy", "gz"), pairs)


def passed_along(x, axis, by):
    count = lax.axis_size(axis)
    pairs = [(i, i + by) for i in range(count) if 0 <= i + by < count]
    return lax.ppermute(x, axis, pairs)


def general(volume, weights, offsets, measured):
    cols, rows, depth = volume.shape
    angles = weights.shape[0]
    taps = weights.shape[1]
    blocks = angles // 8
    shifts = offsets[:, 0]
    wblk = weights.reshape(blocks, 8, taps, cols)
    sblk = shifts.reshape(blocks, 8)

    def project(args):
        wb, sb = args
        spread = jnp.einsum("adc,cyz->adyz", wb, volume, precision=lax.Precision.HIGHEST)
        padded = jnp.pad(spread, ((0, 0), (0, 0), (rows, rows), (0, 0)))

        def project_per_angle(plane, shift):
            window = lax.dynamic_slice_in_dim(plane, shift, 2 * rows + taps - 1, 1)
            total = jnp.zeros((2 * rows, depth), jnp.float32)
            for tap in range(taps):
                total = total + window[tap, tap : tap + 2 * rows]
            return total

        return jax.vmap(project_per_angle)(padded, sb)

    window_rows = lax.map(project, (wblk, sblk)).reshape(angles, 2 * rows, depth)
    lower = window_rows[:, :rows]
    upper = window_rows[:, rows:]
    partial_value = upper + passed_along(lower, "gy", -1)
    summed = lax.psum_scatter(partial_value, "gx", scatter_dimension=0, tiled=True)
    resid_share = summed - measured
    before = passed_along(resid_share, "gy", 1)
    resid_all, before_all = (
        lax.all_gather(resid_share, "gx", axis=0, tiled=True),
        lax.all_gather(before, "gx", axis=0, tiled=True),
    )
    extended = jnp.concatenate([before_all, resid_all], axis=1)
    rblk = extended.reshape(blocks, 8, 2 * rows, depth)

    def backward(grad, args):
        wb, sb, rb = args

        def backward_per_angle(plane, shift):
            start = rows - shift - (taps - 1)
            window = lax.dynamic_slice_in_dim(plane, start, rows + taps - 1, 0)
            return jnp.stack(
                [window[taps - 1 - tap : taps - 1 - tap + rows] for tap in range(taps)]
            )

        sheared = jax.vmap(backward_per_angle)(rb, sb)
        grad = grad + jnp.einsum("adc,adyz->cyz", wb, sheared, precision=lax.Precision.HIGHEST)
        return (grad, None)

    gradient, _ = lax.scan(
        backward, jnp.zeros((cols, rows, depth), jnp.float32), (wblk, sblk, rblk)
    )
    entries = angles * rows * depth * lax.axis_size("gy") * lax.axis_size("gz")
    misfit = lax.psum(jnp.sum(resid_share * resid_share), ("gx", "gy", "gz")) / entries
    return (gradient, resid_share, misfit)


def fits(volume, weights, measured):
    cols, rows, depth = volume.shape
    angles, taps, _ = weights.shape
    groups = lax.axis_size("gy")
    deep, rest = divmod(depth, lax.axis_size("gx") * groups)
    return (
        groups == 2
        and lax.axis_size("gz") == 2
        and lax.axis_size("gx") == 8
        and 2 * rows == LANES
        and depth == LANES
        and rest == 0
        and deep == SUBS
        and cols == 2 * SUBS
        and taps * cols == LANES
        and angles == LANES // 2
        and measured.shape[0] == SUBS
    )


def body(volume, weights, offsets, measured):
    cols, rows, depth = volume.shape
    angles, taps, _ = weights.shape
    if not fits(volume, weights, measured):
        return general(volume, weights, offsets, measured)
    share = measured.shape[0]
    bricks = lax.axis_size("gx")
    groups = lax.axis_size("gy")
    peers = bricks * groups
    deep = depth // peers
    moved = (cols // 2 + share // 2) * deep
    f32 = jnp.float32
    wide = taps * cols
    payload, part = pl.pallas_call(
        pack_kernel,
        out_shape=(pltpu.VMEM((peers, moved, LANES), f32), pltpu.VMEM((angles + SUBS, wide), f32)),
        compiler_params=LIMIT,
        name="pack",
    )(
        off_chip(volume),
        off_chip(measured),
        off_chip(weights.transpose(1, 2, 0).reshape(wide, angles)),
        off_chip(offsets.reshape(1, angles)),
    )
    part = over_planes(part)
    arrived = lax.all_to_all(payload, ("gx", "gy"), 0, 0, tiled=True)
    for axis in ("gz", "gy", "gx"):
        pairs = [(i, i ^ 1) for i in range(lax.axis_size(axis))]
        part = jnp.stack([part, lax.ppermute(part, axis, pairs)])
    prepared = pl.pallas_call(
        prepare_kernel,
        out_shape=(
            pltpu.VMEM((bricks, 2 * angles, 2 * wide), jnp.bfloat16),
            pltpu.VMEM((bricks, wide, 3 * angles), jnp.bfloat16),
            pltpu.VMEM((2 * bricks, LANES), jnp.int32),
        ),
        cost_estimate=cost(1 << 26),
        compiler_params=LIMIT, name="prepare",
    )(on_chip(part))
    dims = (bricks, groups, cols, taps, angles, share, deep)
    payload = pl.pallas_call(
        functools.partial(main_kernel, dims),
        out_shape=pltpu.VMEM((peers, moved + SUBS, LANES), f32),
        scratch_shapes=main_scratch(dims),
        compiler_params=LIMIT, name="both_ways",
    )(on_chip(arrived), *map(on_chip, prepared))
    arrived = lax.all_to_all(payload, ("gx", "gy"), 0, 0, tiled=True)
    entries = angles * rows * depth * groups * lax.axis_size("gz")
    own = jnp.sum(arrived[:, moved:], axis=0)
    other = lax.ppermute(own, "gz", [(0, 1), (1, 0)])
    gradient = pl.pallas_call(
        gradient_kernel,
        out_shape=jax.ShapeDtypeStruct(volume.shape, f32),
        cost_estimate=cost(1 << 24),
        compiler_params=LIMIT,
        name="gradient",
    )(on_chip(arrived))
    resid, misfit = pl.pallas_call(
        functools.partial(residual_kernel, entries),
        out_shape=(jax.ShapeDtypeStruct(measured.shape, f32), jax.ShapeDtypeStruct((1, 1), f32)),
        compiler_params=LIMIT,
        name="residual",
    )(on_chip(arrived), on_chip(own), on_chip(other))
    misfit = misfit.reshape(())
    return gradient, resid, misfit


def solution(mesh):
    in_specs = (P("gx", "gy", "gz"), P(None, None, "gx"), P(None, "gx"), P("gx", "gy", "gz"))
    out_specs = (P("gx", "gy", "gz"), P("gx", "gy", "gz"), P())
    return jax.shard_map(body, mesh=mesh, in_specs=in_specs, out_specs=out_specs, check_vma=False)
```

```python
import functools

import jax
import jax.numpy as jnp
from jax import lax
from jax.experimental import pallas as pl
from jax.experimental.pallas import tpu as pltpu
from jax.sharding import PartitionSpec as P


LANES = 128
SUBS = 8
LIMIT = pltpu.CompilerParams(vmem_limit_bytes=8 << 20)
STRIDE = 72
TOGETHER = 4


def split(x):
    high = x.astype(jnp.bfloat16)
    low = (x - high.astype(jnp.float32)).astype(jnp.bfloat16)
    return high, low


def lane_ids(rows):
    return lax.broadcasted_iota(jnp.int32, (rows, LANES), 1)


def swap(x):
    return pltpu.roll(x, LANES // 2, 1)


def parted(first, second):
    left = lane_ids(first.shape[0]) < LANES // 2
    return jnp.where(left, first, second), swap(jnp.where(left, second, first))


def joined(low, high):
    left = lane_ids(low.shape[0]) < LANES // 2
    high = swap(high)
    return jnp.where(left, low, high), jnp.where(left, high, low)


def pack_kernel(vol_ref, meas_ref, w_ref, off_ref, out_ref, part_ref):
    cols, _, depth = vol_ref.shape
    share = meas_ref.shape[0]
    angles = w_ref.shape[1]
    peers = out_ref.shape[0]
    deep = depth // peers
    second = lax.axis_index("gy")
    part_ref[:angles, :] = w_ref[...].T
    shift = jnp.concatenate([off_ref[...], jnp.zeros((1, LANES - angles), jnp.int32)], axis=1).astype(jnp.float32)
    part_ref[angles:, :] = jnp.broadcast_to(shift, (SUBS, LANES))
    at = 0
    for ref, count in ((vol_ref, cols // 2), (meas_ref, share // 2)):
        for j in range(count):
            pair = jnp.concatenate([ref[j + second * count], ref[j + (1 - second) * count]], axis=0)
            out_ref[:, at : at + deep, :] = pair.T.reshape(peers, deep, LANES)
            at += deep


def prepare_kernel(in_ref, wf_ref, wb_ref, sh_ref):
    rows, wide = in_ref.shape[-2:]
    bricks = sh_ref.shape[0] // 2
    angles = rows - SUBS
    mine = lax.axis_index("gx")
    plane = lax.axis_index("gy") * 2 + lax.axis_index("gz")
    for c in range(2):
        for y in range(2):
            for x in range(2):
                i = mine ^ c ^ (2 * (plane ^ (2 * y + x)))
                w = in_ref[c, y, x, :angles, :]
                high, low = split(w)
                wf_ref[i, :angles, :wide] = high
                wf_ref[i, :angles, wide:] = high
                wf_ref[i, angles:, :wide] = low
                wf_ref[i, angles:, wide:] = jnp.zeros_like(low)
                high, low = split(w.T)
                wb_ref[i, :, :angles] = high
                wb_ref[i, :, angles : 2 * angles] = high
                wb_ref[i, :, 2 * angles :] = low
                row = in_ref[c, y, x, angles : angles + 1, :].astype(jnp.int32)
                sh_ref[pl.ds(i, 1), :] = row
                sh_ref[pl.ds(bricks + i, 1), :] = LANES - row


def three(x):
    high, low = split(x)
    return jnp.concatenate([high, low, high], axis=0)


def main_kernel(dims, in_ref, wf_ref, wb_ref, int_ref, out_ref, *scratch):
    sh_ref, total_ref = scratch[:2]
    turn_refs, sh_sem = scratch[2 : 2 + TOGETHER], scratch[2 + TOGETHER]
    bricks, groups, cols, taps, angles, share, deep = dims
    half, quarter = cols // 2, share // 2
    m_at = half * deep
    w_at = m_at + quarter * deep

    to_scalars = pltpu.make_async_copy(int_ref, sh_ref, sh_sem)
    to_scalars.start()
    total_ref[...] = jnp.zeros_like(total_ref)
    lane_c = lane_ids(cols)
    lane = lane_ids(deep)
    zero = jnp.zeros((cols, LANES), jnp.bfloat16)

    def project(i, turn_ref):
        for q in range(deep // 2):
            blocks = []
            for z in (2 * q, 2 * q + 1):
                first, second = (in_ref[i * groups + h, pl.ds(z, half, stride=deep), :] for h in range(2))
                x = jnp.concatenate(parted(first, second), axis=0)
                parts = []
                for part in split(x):
                    moved = [part]
                    for tap in range(1, taps):
                        moved.append(jnp.where(lane_c < LANES - tap, pltpu.roll(part, LANES - tap, 1), zero))
                    parts.append(jnp.concatenate(moved, axis=0))
                blocks.append(jnp.concatenate(parts, axis=0))
            out = jnp.dot(wf_ref[i], jnp.concatenate(blocks, axis=1), preferred_element_type=jnp.float32)
            out = out[:angles] + out[angles:]
            for k in range(2):
                at = (2 * q + k) * STRIDE
                turn_ref[at : at + angles, :] = out[:, k * LANES : (k + 1) * LANES]

    def gather_rows(i, turn_refs):
        for a in range(angles):
            part = total_ref[a]
            for k, turn_ref in enumerate(turn_refs):
                reach = sh_ref[bricks + i + k, a]
                moved = pltpu.roll(turn_ref[pl.ds(a, deep, stride=STRIDE), :], reach, 1)
                part = part + jnp.where(lane < reach, moved, 0.0)
            total_ref[a] = part

    def forward(n, carry):
        i = n * TOGETHER
        for k, turn_ref in enumerate(turn_refs):
            project(i + k, turn_ref)

        @pl.when(n == 0)
        def _():
            to_scalars.wait()

        gather_rows(i, turn_refs)
        return carry

    def scatter_rows(i, turn_ref):
        for a in range(angles):
            shift = sh_ref[i, a]
            turn_ref[pl.ds(a, deep, stride=STRIDE), :] = jnp.where(lane >= shift, pltpu.roll(total_ref[a], shift, 1), 0.0)

    def backproject(i, turn_ref):
        for q in range(deep // 2):
            zs = (2 * q, 2 * q + 1)
            blocks = [three(turn_ref[z * STRIDE : z * STRIDE + angles, :]) for z in zs]
            out = jnp.dot(wb_ref[i], jnp.concatenate(blocks, axis=1), preferred_element_type=jnp.float32)
            for k, z in enumerate(zs):
                part = out[:, k * LANES : (k + 1) * LANES]
                total = part[:cols]
                for tap in range(1, taps):
                    total = total + jnp.where(lane_c >= tap, pltpu.roll(part[tap * cols : (tap + 1) * cols], tap, 1), 0.0)
                for h, block in enumerate(joined(total[:half], total[half:])):
                    out_ref[i * groups + h, pl.ds(z, half, stride=deep), :] = block

    def backward(n, carry):
        i = 2 * n
        for k in range(2):
            scatter_rows(i + k, turn_refs[k])
            backproject(i + k, turn_refs[k])
        return carry

    lax.fori_loop(0, bricks // TOGETHER, forward, 0)
    square = jnp.zeros((deep, LANES), jnp.float32)
    for i in range(bricks):
        for j in range(quarter):
            at = m_at + j * deep
            low_at, high_at = i * share + j, i * share + quarter + j
            low, high = parted(*(in_ref[i * groups + h, at : at + deep, :] for h in range(2)))
            low, high = total_ref[low_at] - low, total_ref[high_at] - high
            total_ref[low_at], total_ref[high_at] = low, high
            square = square + low * low + high * high
            for h, block in enumerate(joined(low, high)):
                out_ref[i * groups + h, at : at + deep, :] = block
    for p in range(bricks * groups):
        out_ref[p, w_at : w_at + deep, :] = square
    lax.fori_loop(0, bricks // 2, backward, 0)


def main_scratch(dims):
    bricks, _, _, _, angles, _, deep = dims
    f32 = jnp.float32
    return [
        pltpu.SMEM((2 * bricks, LANES), jnp.int32),
        pltpu.VMEM((angles, deep, LANES), f32),
        *[pltpu.VMEM((deep * STRIDE, LANES), f32) for _ in range(TOGETHER)],
        pltpu.SemaphoreType.DMA,
    ]


def unpack(in_ref, at, out_ref):
    peers = in_ref.shape[0]
    count, rows, depth = out_ref.shape
    deep = depth // peers
    second = lax.axis_index("gy")
    for j in range(count // 2):
        both = in_ref[:, at : at + deep, :].reshape(depth, LANES).T
        out_ref[j + second * (count // 2)] = both[:rows]
        out_ref[j + (1 - second) * (count // 2)] = both[rows:]
        at += deep


def unpack_kernel(in_ref, grad_ref, res_ref):
    unpack(in_ref, 0, grad_ref)
    unpack(in_ref, grad_ref.shape[0] // 2 * (grad_ref.shape[2] // in_ref.shape[0]), res_ref)


def misfit_kernel(entries, own_ref, other_ref, out_ref):
    out_ref[...] = jnp.sum(own_ref[...] + other_ref[...], keepdims=True) / entries


def cost(flops):
    return pl.CostEstimate(flops=flops, bytes_accessed=1 << 21, transcendentals=0)


def off_chip(x):
    return pltpu.with_memory_space_constraint(x, pltpu.HBM)


def on_chip(x):
    return pltpu.with_memory_space_constraint(x, pltpu.VMEM)


def over_planes(x):
    sizes = [lax.axis_size(axis) for axis in ("gx", "gy", "gz")]
    planes = sizes[1] * sizes[2]
    pairs = [(at * planes + q, (at ^ (2 * q)) * planes + q) for at in range(sizes[0]) for q in range(planes)]
    return lax.ppermute(x, ("gx", "gy", "gz"), pairs)


def passed_along(x, axis, by):
    count = lax.axis_size(axis)
    pairs = [(i, i + by) for i in range(count) if 0 <= i + by < count]
    return lax.ppermute(x, axis, pairs)


def general(volume, weights, offsets, measured):
    cols, rows, depth = volume.shape
    angles = weights.shape[0]
    taps = weights.shape[1]
    blocks = angles // 8
    shifts = offsets[:, 0]
    wblk = weights.reshape(blocks, 8, taps, cols)
    sblk = shifts.reshape(blocks, 8)

    def project(args):
        wb, sb = args
        spread = jnp.einsum("adc,cyz->adyz", wb, volume, precision=lax.Precision.HIGHEST)
        padded = jnp.pad(spread, ((0, 0), (0, 0), (rows, rows), (0, 0)))

        def project_per_angle(plane, shift):
            window = lax.dynamic_slice_in_dim(plane, shift, 2 * rows + taps - 1, 1)
            total = jnp.zeros((2 * rows, depth), jnp.float32)
            for tap in range(taps):
                total = total + window[tap, tap : tap + 2 * rows]
            return total

        return jax.vmap(project_per_angle)(padded, sb)

    window_rows = lax.map(project, (wblk, sblk)).reshape(angles, 2 * rows, depth)
    lower = window_rows[:, :rows]
    upper = window_rows[:, rows:]
    partial_value = upper + passed_along(lower, "gy", -1)
    summed = lax.psum_scatter(partial_value, "gx", scatter_dimension=0, tiled=True)
    resid_share = summed - measured
    before = passed_along(resid_share, "gy", 1)
    resid_all, before_all = (
        lax.all_gather(resid_share, "gx", axis=0, tiled=True),
        lax.all_gather(before, "gx", axis=0, tiled=True),
    )
    extended = jnp.concatenate([before_all, resid_all], axis=1)
    rblk = extended.reshape(blocks, 8, 2 * rows, depth)

    def backward(grad, args):
        wb, sb, rb = args

        def backward_per_angle(plane, shift):
            start = rows - shift - (taps - 1)
            window = lax.dynamic_slice_in_dim(plane, start, rows + taps - 1, 0)
            return jnp.stack(
                [window[taps - 1 - tap : taps - 1 - tap + rows] for tap in range(taps)]
            )

        sheared = jax.vmap(backward_per_angle)(rb, sb)
        grad = grad + jnp.einsum("adc,adyz->cyz", wb, sheared, precision=lax.Precision.HIGHEST)
        return (grad, None)

    gradient, _ = lax.scan(
        backward, jnp.zeros((cols, rows, depth), jnp.float32), (wblk, sblk, rblk)
    )
    entries = angles * rows * depth * lax.axis_size("gy") * lax.axis_size("gz")
    misfit = lax.psum(jnp.sum(resid_share * resid_share), ("gx", "gy", "gz")) / entries
    return (gradient, resid_share, misfit)


def fits(volume, weights, measured):
    cols, rows, depth = volume.shape
    angles, taps, _ = weights.shape
    groups = lax.axis_size("gy")
    deep, rest = divmod(depth, lax.axis_size("gx") * groups)
    return (
        groups == 2
        and lax.axis_size("gz") == 2
        and lax.axis_size("gx") == 2 * groups * lax.axis_size("gz")
        and 2 * rows == LANES
        and depth == LANES
        and rest == 0
        and deep == SUBS
        and cols == 2 * SUBS
        and taps * cols == LANES
        and angles == LANES // 2
        and measured.shape[0] == SUBS
    )


def body(volume, weights, offsets, measured):
    cols, rows, depth = volume.shape
    angles, taps, _ = weights.shape
    if not fits(volume, weights, measured):
        return general(volume, weights, offsets, measured)
    share = measured.shape[0]
    bricks = lax.axis_size("gx")
    groups = lax.axis_size("gy")
    peers = bricks * groups
    deep = depth // peers
    moved = (cols // 2 + share // 2) * deep
    f32 = jnp.float32
    wide = taps * cols
    payload, part = pl.pallas_call(
        pack_kernel,
        out_shape=(pltpu.VMEM((peers, moved, LANES), f32), pltpu.VMEM((angles + SUBS, wide), f32)),
        compiler_params=LIMIT,
        name="pack",
    )(
        off_chip(volume),
        off_chip(measured),
        off_chip(weights.transpose(1, 2, 0).reshape(wide, angles)),
        off_chip(offsets.reshape(1, angles)),
    )
    part = over_planes(part)
    arrived = lax.all_to_all(payload, ("gx", "gy"), 0, 0, tiled=True)
    for axis in ("gz", "gy", "gx"):
        pairs = [(i, i ^ 1) for i in range(lax.axis_size(axis))]
        part = jnp.stack([part, lax.ppermute(part, axis, pairs)])
    prepared = pl.pallas_call(
        prepare_kernel,
        out_shape=(
            pltpu.VMEM((bricks, 2 * angles, 2 * wide), jnp.bfloat16),
            pltpu.VMEM((bricks, wide, 3 * angles), jnp.bfloat16),
            pltpu.VMEM((2 * bricks, LANES), jnp.int32),
        ),
        cost_estimate=cost(1 << 26),
        compiler_params=LIMIT, name="prepare",
    )(on_chip(part))
    dims = (bricks, groups, cols, taps, angles, share, deep)
    payload = pl.pallas_call(
        functools.partial(main_kernel, dims),
        out_shape=pltpu.VMEM((peers, moved + SUBS, LANES), f32),
        scratch_shapes=main_scratch(dims),
        compiler_params=LIMIT, name="both_ways",
    )(on_chip(arrived), *map(on_chip, prepared))
    arrived = lax.all_to_all(payload, ("gx", "gy"), 0, 0, tiled=True)
    entries = angles * rows * depth * groups * lax.axis_size("gz")
    own = jnp.sum(arrived[:, moved:], axis=0)
    other = lax.ppermute(own, "gz", [(0, 1), (1, 0)])
    gradient, resid = pl.pallas_call(
        unpack_kernel,
        out_shape=(jax.ShapeDtypeStruct(volume.shape, f32), jax.ShapeDtypeStruct(measured.shape, f32)),
        cost_estimate=cost(1 << 24),
        compiler_params=LIMIT,
        name="unpack",
    )(on_chip(arrived))
    misfit = pl.pallas_call(
        functools.partial(misfit_kernel, entries),
        out_shape=jax.ShapeDtypeStruct((1, 1), f32),
        compiler_params=LIMIT,
        name="misfit",
    )(on_chip(own), on_chip(other))
    misfit = misfit.reshape(())
    return gradient, resid, misfit


def solution(mesh):
    in_specs = (P("gx", "gy", "gz"), P(None, None, "gx"), P(None, "gx"), P("gx", "gy", "gz"))
    out_specs = (P("gx", "gy", "gz"), P("gx", "gy", "gz"), P())
    return jax.shard_map(body, mesh=mesh, in_specs=in_specs, out_specs=out_specs, check_vma=False)
```

```python
import functools

import jax
import jax.numpy as jnp
from jax import lax
from jax.experimental import pallas as pl
from jax.experimental.pallas import tpu as pltpu
from jax.sharding import PartitionSpec as P


LANES = 128
SUBS = 8
LIMIT = pltpu.CompilerParams(vmem_limit_bytes=8 << 20)
STRIDE = 72
TOGETHER = 4
BACK = 4


def split(x):
    high = x.astype(jnp.bfloat16)
    low = (x - high.astype(jnp.float32)).astype(jnp.bfloat16)
    return high, low


def lane_ids(rows):
    return lax.broadcasted_iota(jnp.int32, (rows, LANES), 1)


def swap(x):
    return pltpu.roll(x, LANES // 2, 1)


def parted(first, second):
    left = lane_ids(first.shape[0]) < LANES // 2
    return jnp.where(left, first, second), swap(jnp.where(left, second, first))


def joined(low, high):
    left = lane_ids(low.shape[0]) < LANES // 2
    high = swap(high)
    return jnp.where(left, low, high), jnp.where(left, high, low)


def pack_kernel(vol_ref, meas_ref, w_ref, off_ref, out_ref, part_ref):
    cols, _, depth = vol_ref.shape
    share = meas_ref.shape[0]
    angles = w_ref.shape[1]
    peers = out_ref.shape[0]
    deep = depth // peers
    second = lax.axis_index("gy")
    part_ref[:angles, :] = w_ref[...].T
    shift = jnp.concatenate([off_ref[...], jnp.zeros((1, LANES - angles), jnp.int32)], axis=1).astype(jnp.float32)
    part_ref[angles:, :] = jnp.broadcast_to(shift, (SUBS, LANES))
    at = 0
    for ref, count in ((vol_ref, cols // 2), (meas_ref, share // 2)):
        for j in range(count):
            pair = jnp.concatenate([ref[j + second * count], ref[j + (1 - second) * count]], axis=0)
            out_ref[:, at : at + deep, :] = pair.T.reshape(peers, deep, LANES)
            at += deep


def prepare_kernel(in_ref, wf_ref, wb_ref, sh_ref):
    rows, wide = in_ref.shape[-2:]
    bricks = sh_ref.shape[0] // 2
    angles = rows - SUBS
    mine = lax.axis_index("gx")
    plane = lax.axis_index("gy") * 2 + lax.axis_index("gz")
    for c in range(2):
        for y in range(2):
            for x in range(2):
                i = mine ^ c ^ (2 * (plane ^ (2 * y + x)))
                w = in_ref[c, y, x, :angles, :]
                high, low = split(w)
                wf_ref[i, :angles, :wide] = high
                wf_ref[i, :angles, wide:] = high
                wf_ref[i, angles:, :wide] = low
                wf_ref[i, angles:, wide:] = jnp.zeros_like(low)
                high, low = split(w.T)
                wb_ref[i, :, :angles] = high
                wb_ref[i, :, angles : 2 * angles] = high
                wb_ref[i, :, 2 * angles :] = low
                row = in_ref[c, y, x, angles : angles + 1, :].astype(jnp.int32)
                sh_ref[pl.ds(i, 1), :] = row
                sh_ref[pl.ds(bricks + i, 1), :] = LANES - row


def three(x):
    high, low = split(x)
    return jnp.concatenate([high, low, high], axis=0)


def main_kernel(dims, in_ref, wf_ref, wb_ref, int_ref, out_ref, *scratch):
    sh_ref, total_ref = scratch[:2]
    turn_refs, sh_sem = scratch[2 : 2 + TOGETHER], scratch[2 + TOGETHER]
    bricks, groups, cols, taps, angles, share, deep = dims
    half, quarter = cols // 2, share // 2
    m_at = half * deep
    w_at = m_at + quarter * deep

    to_scalars = pltpu.make_async_copy(int_ref, sh_ref, sh_sem)
    to_scalars.start()
    total_ref[...] = jnp.zeros_like(total_ref)
    lane_c = lane_ids(cols)
    lane = lane_ids(deep)
    zero = jnp.zeros((cols, LANES), jnp.bfloat16)

    def project(i, turn_ref):
        for q in range(deep // 2):
            blocks = []
            for z in (2 * q, 2 * q + 1):
                first, second = (in_ref[i * groups + h, pl.ds(z, half, stride=deep), :] for h in range(2))
                x = jnp.concatenate(parted(first, second), axis=0)
                parts = []
                for part in split(x):
                    moved = [part]
                    for tap in range(1, taps):
                        moved.append(jnp.where(lane_c < LANES - tap, pltpu.roll(part, LANES - tap, 1), zero))
                    parts.append(jnp.concatenate(moved, axis=0))
                blocks.append(jnp.concatenate(parts, axis=0))
            out = jnp.dot(wf_ref[i], jnp.concatenate(blocks, axis=1), preferred_element_type=jnp.float32)
            out = out[:angles] + out[angles:]
            for k in range(2):
                at = (2 * q + k) * STRIDE
                turn_ref[at : at + angles, :] = out[:, k * LANES : (k + 1) * LANES]

    def gather_rows(i, turn_refs):
        for a in range(angles):
            part = total_ref[a]
            for k, turn_ref in enumerate(turn_refs):
                reach = sh_ref[bricks + i + k, a]
                moved = pltpu.roll(turn_ref[pl.ds(a, deep, stride=STRIDE), :], reach, 1)
                part = part + jnp.where(lane < reach, moved, 0.0)
            total_ref[a] = part

    def forward(n, carry):
        i = n * TOGETHER
        for k, turn_ref in enumerate(turn_refs):
            project(i + k, turn_ref)

        @pl.when(n == 0)
        def _():
            to_scalars.wait()

        gather_rows(i, turn_refs)
        return carry

    def scatter_rows(i, turn_ref):
        for a in range(angles):
            shift = sh_ref[i, a]
            turn_ref[pl.ds(a, deep, stride=STRIDE), :] = jnp.where(lane >= shift, pltpu.roll(total_ref[a], shift, 1), 0.0)

    def backproject(i, turn_ref):
        for q in range(deep // 2):
            zs = (2 * q, 2 * q + 1)
            blocks = [three(turn_ref[z * STRIDE : z * STRIDE + angles, :]) for z in zs]
            out = jnp.dot(wb_ref[i], jnp.concatenate(blocks, axis=1), preferred_element_type=jnp.float32)
            for k, z in enumerate(zs):
                part = out[:, k * LANES : (k + 1) * LANES]
                total = part[:cols]
                for tap in range(1, taps):
                    total = total + jnp.where(lane_c >= tap, pltpu.roll(part[tap * cols : (tap + 1) * cols], tap, 1), 0.0)
                for h, block in enumerate(joined(total[:half], total[half:])):
                    out_ref[i * groups + h, pl.ds(z, half, stride=deep), :] = block

    lax.fori_loop(0, bricks // TOGETHER, forward, 0)
    square = jnp.zeros((deep, LANES), jnp.float32)
    for i in range(bricks):
        for j in range(quarter):
            at = m_at + j * deep
            low_at, high_at = i * share + j, i * share + quarter + j
            low, high = parted(*(in_ref[i * groups + h, at : at + deep, :] for h in range(2)))
            low, high = total_ref[low_at] - low, total_ref[high_at] - high
            total_ref[low_at], total_ref[high_at] = low, high
            square = square + low * low + high * high
            for h, block in enumerate(joined(low, high)):
                out_ref[i * groups + h, at : at + deep, :] = block

    def backward(n, carry):
        i = n * BACK
        for k in range(BACK):
            scatter_rows(i + k, turn_refs[k])

        @pl.when(n == 0)
        def _():
            for p in range(bricks * groups):
                out_ref[p, w_at : w_at + deep, :] = square

        for k in range(BACK):
            backproject(i + k, turn_refs[k])
        return carry

    lax.fori_loop(0, bricks // BACK, backward, 0)


def main_scratch(dims):
    bricks, _, _, _, angles, _, deep = dims
    f32 = jnp.float32
    return [
        pltpu.SMEM((2 * bricks, LANES), jnp.int32),
        pltpu.VMEM((angles, deep, LANES), f32),
        *[pltpu.VMEM((deep * STRIDE, LANES), f32) for _ in range(TOGETHER)],
        pltpu.SemaphoreType.DMA,
    ]


def unpack(in_ref, at, out_ref):
    peers = in_ref.shape[0]
    count, rows, depth = out_ref.shape
    deep = depth // peers
    second = lax.axis_index("gy")
    for j in range(count // 2):
        both = in_ref[:, at : at + deep, :].reshape(depth, LANES).T
        out_ref[j + second * (count // 2)] = both[:rows]
        out_ref[j + (1 - second) * (count // 2)] = both[rows:]
        at += deep


def unpack_kernel(in_ref, grad_ref, res_ref):
    unpack(in_ref, 0, grad_ref)
    unpack(in_ref, grad_ref.shape[0] // 2 * (grad_ref.shape[2] // in_ref.shape[0]), res_ref)


def misfit_kernel(entries, own_ref, other_ref, out_ref):
    out_ref[...] = jnp.sum(own_ref[...] + other_ref[...], keepdims=True) / entries


def cost(flops):
    return pl.CostEstimate(flops=flops, bytes_accessed=1 << 21, transcendentals=0)


def off_chip(x):
    return pltpu.with_memory_space_constraint(x, pltpu.HBM)


def on_chip(x):
    return pltpu.with_memory_space_constraint(x, pltpu.VMEM)


def over_planes(x):
    sizes = [lax.axis_size(axis) for axis in ("gx", "gy", "gz")]
    planes = sizes[1] * sizes[2]
    pairs = [(at * planes + q, (at ^ (2 * q)) * planes + q) for at in range(sizes[0]) for q in range(planes)]
    return lax.ppermute(x, ("gx", "gy", "gz"), pairs)


def passed_along(x, axis, by):
    count = lax.axis_size(axis)
    pairs = [(i, i + by) for i in range(count) if 0 <= i + by < count]
    return lax.ppermute(x, axis, pairs)


def general(volume, weights, offsets, measured):
    cols, rows, depth = volume.shape
    angles = weights.shape[0]
    taps = weights.shape[1]
    blocks = angles // 8
    shifts = offsets[:, 0]
    wblk = weights.reshape(blocks, 8, taps, cols)
    sblk = shifts.reshape(blocks, 8)

    def project(args):
        wb, sb = args
        spread = jnp.einsum("adc,cyz->adyz", wb, volume, precision=lax.Precision.HIGHEST)
        padded = jnp.pad(spread, ((0, 0), (0, 0), (rows, rows), (0, 0)))

        def project_per_angle(plane, shift):
            window = lax.dynamic_slice_in_dim(plane, shift, 2 * rows + taps - 1, 1)
            total = jnp.zeros((2 * rows, depth), jnp.float32)
            for tap in range(taps):
                total = total + window[tap, tap : tap + 2 * rows]
            return total

        return jax.vmap(project_per_angle)(padded, sb)

    window_rows = lax.map(project, (wblk, sblk)).reshape(angles, 2 * rows, depth)
    lower = window_rows[:, :rows]
    upper = window_rows[:, rows:]
    partial_value = upper + passed_along(lower, "gy", -1)
    summed = lax.psum_scatter(partial_value, "gx", scatter_dimension=0, tiled=True)
    resid_share = summed - measured
    before = passed_along(resid_share, "gy", 1)
    resid_all, before_all = (
        lax.all_gather(resid_share, "gx", axis=0, tiled=True),
        lax.all_gather(before, "gx", axis=0, tiled=True),
    )
    extended = jnp.concatenate([before_all, resid_all], axis=1)
    rblk = extended.reshape(blocks, 8, 2 * rows, depth)

    def backward(grad, args):
        wb, sb, rb = args

        def backward_per_angle(plane, shift):
            start = rows - shift - (taps - 1)
            window = lax.dynamic_slice_in_dim(plane, start, rows + taps - 1, 0)
            return jnp.stack(
                [window[taps - 1 - tap : taps - 1 - tap + rows] for tap in range(taps)]
            )

        sheared = jax.vmap(backward_per_angle)(rb, sb)
        grad = grad + jnp.einsum("adc,adyz->cyz", wb, sheared, precision=lax.Precision.HIGHEST)
        return (grad, None)

    gradient, _ = lax.scan(
        backward, jnp.zeros((cols, rows, depth), jnp.float32), (wblk, sblk, rblk)
    )
    entries = angles * rows * depth * lax.axis_size("gy") * lax.axis_size("gz")
    misfit = lax.psum(jnp.sum(resid_share * resid_share), ("gx", "gy", "gz")) / entries
    return (gradient, resid_share, misfit)


def fits(volume, weights, measured):
    cols, rows, depth = volume.shape
    angles, taps, _ = weights.shape
    groups = lax.axis_size("gy")
    deep, rest = divmod(depth, lax.axis_size("gx") * groups)
    return (
        groups == 2
        and lax.axis_size("gz") == 2
        and lax.axis_size("gx") == 2 * groups * lax.axis_size("gz")
        and 2 * rows == LANES
        and depth == LANES
        and rest == 0
        and deep == SUBS
        and cols == 2 * SUBS
        and taps * cols == LANES
        and angles == LANES // 2
        and measured.shape[0] == SUBS
    )


def body(volume, weights, offsets, measured):
    cols, rows, depth = volume.shape
    angles, taps, _ = weights.shape
    if not fits(volume, weights, measured):
        return general(volume, weights, offsets, measured)
    share = measured.shape[0]
    bricks = lax.axis_size("gx")
    groups = lax.axis_size("gy")
    peers = bricks * groups
    deep = depth // peers
    moved = (cols // 2 + share // 2) * deep
    f32 = jnp.float32
    wide = taps * cols
    payload, part = pl.pallas_call(
        pack_kernel,
        out_shape=(pltpu.VMEM((peers, moved, LANES), f32), pltpu.VMEM((angles + SUBS, wide), f32)),
        compiler_params=LIMIT,
        name="pack",
    )(
        off_chip(volume),
        off_chip(measured),
        off_chip(weights.transpose(1, 2, 0).reshape(wide, angles)),
        off_chip(offsets.reshape(1, angles)),
    )
    part = over_planes(part)
    arrived = lax.all_to_all(payload, ("gx", "gy"), 0, 0, tiled=True)
    for axis in ("gz", "gy", "gx"):
        pairs = [(i, i ^ 1) for i in range(lax.axis_size(axis))]
        part = jnp.stack([part, lax.ppermute(part, axis, pairs)])
    prepared = pl.pallas_call(
        prepare_kernel,
        out_shape=(
            pltpu.VMEM((bricks, 2 * angles, 2 * wide), jnp.bfloat16),
            pltpu.VMEM((bricks, wide, 3 * angles), jnp.bfloat16),
            pltpu.VMEM((2 * bricks, LANES), jnp.int32),
        ),
        cost_estimate=cost(1 << 26),
        compiler_params=LIMIT, name="prepare",
    )(on_chip(part))
    dims = (bricks, groups, cols, taps, angles, share, deep)
    payload = pl.pallas_call(
        functools.partial(main_kernel, dims),
        out_shape=pltpu.VMEM((peers, moved + SUBS, LANES), f32),
        scratch_shapes=main_scratch(dims),
        compiler_params=LIMIT, name="both_ways",
    )(on_chip(arrived), *map(on_chip, prepared))
    arrived = lax.all_to_all(payload, ("gx", "gy"), 0, 0, tiled=True)
    entries = angles * rows * depth * groups * lax.axis_size("gz")
    own = jnp.sum(arrived[:, moved:], axis=0)
    other = lax.ppermute(own, "gz", [(0, 1), (1, 0)])
    gradient, resid = pl.pallas_call(
        unpack_kernel,
        out_shape=(jax.ShapeDtypeStruct(volume.shape, f32), jax.ShapeDtypeStruct(measured.shape, f32)),
        cost_estimate=cost(1 << 24),
        compiler_params=LIMIT,
        name="unpack",
    )(on_chip(arrived))
    misfit = pl.pallas_call(
        functools.partial(misfit_kernel, entries),
        out_shape=jax.ShapeDtypeStruct((1, 1), f32),
        compiler_params=LIMIT,
        name="misfit",
    )(on_chip(own), on_chip(other))
    misfit = misfit.reshape(())
    return gradient, resid, misfit


def solution(mesh):
    in_specs = (P("gx", "gy", "gz"), P(None, None, "gx"), P(None, "gx"), P("gx", "gy", "gz"))
    out_specs = (P("gx", "gy", "gz"), P("gx", "gy", "gz"), P())
    return jax.shard_map(body, mesh=mesh, in_specs=in_specs, out_specs=out_specs, check_vma=False)
```
